64 devices in a mesh: data: 4 (over x, y), expert: 16 (over z, core).
Axes of the slice: x: 2, y: 2, z: 8, core: 2. Of those that a mesh axis runs over, the one named last changes fastest.
The devices are a block of a 4x4x8 slice.
Arguments:
- x_tok: bfloat16 [4096, 2048], P(('data', 'expert')), parts along dimension 0
- topk_idx: int32 [4096, 6], P(('data', 'expert')), parts along dimension 0
- topk_w: float32 [4096, 6], P(('data', 'expert')), parts along dimension 0
- w_up: bfloat16 [64, 2048, 1408], P('expert')
- w_down: bfloat16 [64, 1408, 2048], P('expert')
Outputs:
- output: bfloat16 [4096, 2048], P(('data', 'expert')), parts along dimension 0
There are 4 independent parts. The reference program is written for one: setup_inputs(seed, part) draws one part's arguments, and reference() takes and returns one part's arrays. A program takes and returns all parts, laid end to end along the dimension named above; an argument that names none is the same for every part.
All inputs are finite; a program needn't handle non-finite values.
Results may differ from the reference program's by a relative error of at most 0.0013.
Values are sent between devices in bfloat16 or wider.
A program may use at most 768 MiB of HBM per device.

```python
import jax
import jax.numpy as jnp
from jax import lax

D_MODEL = 2048
D_FF = 1408
EXPERTS = 64
TOP_K = 6
TOK_DEV = 64
GROUP_SIZE = 16
HOT_MUL = min(4, EXPERTS // TOP_K)
SLOT_CAP = HOT_MUL * TOK_DEV * TOP_K // EXPERTS
NUM_HOT = max(1, EXPERTS // 32)
TOKENS = GROUP_SIZE * TOK_DEV


def draw_routing(key):
    hot_key, dev_key = jax.random.split(key)
    exp_perm = jax.random.permutation(hot_key, EXPERTS)
    n_cold = EXPERTS - NUM_HOT
    cold_total = TOK_DEV * TOP_K - NUM_HOT * SLOT_CAP
    base_count = cold_total // n_cold
    extra_count = cold_total - base_count * n_cold

    def one_device(dev_seed):
        shift_key, order_key, perm_key = jax.random.split(dev_seed, 3)
        shifts = jax.random.randint(shift_key, (n_cold // 2,), 0, base_count // 2 + 1)
        count_shift = jnp.concatenate([jnp.stack([shifts, -shifts], axis=1).reshape(-1), jnp.zeros((n_cold % 2,), jnp.int32)])
        cold_counts = base_count + (jnp.arange(n_cold) < extra_count).astype(jnp.int32) + count_shift
        counts = jnp.concatenate([jnp.full((NUM_HOT,), SLOT_CAP, jnp.int32), cold_counts])
        visit_order = jax.random.permutation(order_key, EXPERTS)
        run_ends = jnp.cumsum(counts[visit_order])
        run_index = jnp.searchsorted(run_ends, jnp.arange(TOK_DEV * TOP_K), side='right')
        pair_seq = exp_perm[visit_order][run_index]
        choice = pair_seq.reshape(TOP_K, TOK_DEV).T
        return choice[jax.random.permutation(perm_key, TOK_DEV)]

    dev_keys = jax.random.split(dev_key, GROUP_SIZE)
    return jax.vmap(one_device)(dev_keys).reshape(TOKENS, TOP_K).astype(jnp.int32)


def setup_inputs(seed: int = 0, part: int = 0) -> dict:
    part_key = jax.random.fold_in(jax.random.key(seed), part)
    route_key, gate_key, tok_key = jax.random.split(part_key, 3)
    up_key, down_key = jax.random.split(jax.random.key(seed + 1))
    x_tok = jax.random.normal(tok_key, (TOKENS, D_MODEL), jnp.float32).astype(jnp.bfloat16)
    topk_idx = draw_routing(route_key)
    topk_w = jax.random.uniform(gate_key, (TOKENS, TOP_K), jnp.float32, 0.1, 1.0)
    w_up = (jax.random.normal(up_key, (EXPERTS, D_MODEL, D_FF), jnp.float32) * D_MODEL ** -0.5).astype(jnp.bfloat16)
    w_down = (jax.random.normal(down_key, (EXPERTS, D_FF, D_MODEL), jnp.float32) * D_FF ** -0.5).astype(jnp.bfloat16)
    return {'x_tok': x_tok, 'topk_idx': topk_idx, 'topk_w': topk_w, 'w_up': w_up, 'w_down': w_down}


def reference(x_tok, topk_idx, topk_w, w_up, w_down):
    pair_exp = topk_idx.reshape(-1)
    n_pairs = TOKENS * TOP_K
    group_cap = GROUP_SIZE * SLOT_CAP
    sort_order = jnp.argsort(pair_exp, stable=True)
    pair_rank = jnp.argsort(sort_order, stable=True)
    counts = jnp.bincount(pair_exp, length=EXPERTS)
    starts = jnp.cumsum(counts) - counts
    slot_src = jnp.minimum(starts[:, None] + jnp.arange(group_cap)[None, :], n_pairs - 1)
    slot_tok = sort_order[slot_src] // TOP_K

    def expert_rows(operands):
        tok_ids, up_mat, down_mat = operands
        tok_rows = x_tok[tok_ids]
        hidden = jnp.dot(tok_rows, up_mat, preferred_element_type=jnp.float32)
        hidden = jax.nn.gelu(hidden, approximate=True).astype(jnp.bfloat16)
        return jnp.dot(hidden, down_mat, preferred_element_type=jnp.float32).astype(jnp.bfloat16)

    slot_out = lax.map(expert_rows, (slot_tok, w_up, w_down)).reshape(EXPERTS * group_cap, D_MODEL)
    pair_slot = pair_exp * group_cap + pair_rank - starts[pair_exp]
    pair_out = slot_out[pair_slot].reshape(TOKENS, TOP_K, D_MODEL)
    y_tok = jnp.sum(topk_w[:, :, None] * pair_out.astype(jnp.float32), axis=1)
    return y_tok.astype(jnp.bfloat16)
```

```python
import functools

import jax
import jax.numpy as jnp
from jax import lax
from jax.experimental import pallas as pl
from jax.experimental.pallas import tpu as pltpu
from jax.sharding import PartitionSpec as P

MESH = pl.DeviceIdType.MESH
COLS = 256
LANES = 128
WD_SLOTS = 3


def moe_kernel(group, cap, x_hbm, meta_hbm, up_hbm, down_hbm, y_ref,
               wup, wd, xb, metab, xg, hid, cmat, ob, acc, psend, precv, rhalf, rfull,
               loc_sem, up_sem, wd_sem, ag_s, ag_r, mt_s, mt_r, pd_s, pd_r, pm_s, pm_r,
               ps_s, ps_r, h_s, h_r, f_s, f_r):
    n_chip = group // 2
    hops = n_chip // 2
    n_exp, d_model, d_ff = wup.shape
    tok = xb.shape[2]
    half = tok // 2
    chip_cap = 2 * cap
    slots = n_exp * chip_cap
    n_col = d_model // COLS
    f32, bf16 = jnp.float32, jnp.bfloat16

    me = lax.axis_index('expert')
    chip, core = me // 2, me % 2
    right = lax.rem(chip + 1, n_chip) * 2 + core
    left = lax.rem(chip + n_chip - 1, n_chip) * 2 + core
    partner = chip * 2 + 1 - core

    def remote(src, dst, send_sem, recv_sem, dev):
        return pltpu.make_async_remote_copy(src_ref=src, dst_ref=dst, send_sem=send_sem, recv_sem=recv_sem,
                                            device_id={'expert': dev}, device_id_type=MESH)

    x_copy = pltpu.make_async_copy(x_hbm, xb.at[0, 0], loc_sem.at[0])
    m_copy = pltpu.make_async_copy(meta_hbm, metab.at[0, 0], loc_sem.at[1])
    x_copy.start()
    m_copy.start()

    def up_copy(e):
        return pltpu.make_async_copy(up_hbm.at[e], wup.at[e], up_sem.at[e])

    def wd_copy(c):
        slot = lax.rem(c, WD_SLOTS)
        cols = pl.ds(pl.multiple_of(c * COLS, COLS), COLS)
        return pltpu.make_async_copy(down_hbm.at[:, :, cols], wd.at[slot], wd_sem.at[slot])

    for e in range(n_exp):
        up_copy(e).start()
    for c in range(min(WD_SLOTS, n_col)):
        wd_copy(jnp.int32(c)).start()

    barrier = pltpu.get_barrier_semaphore()
    for dev in (right, left, partner):
        pl.semaphore_signal(barrier, inc=1, device_id={'expert': dev}, device_id_type=MESH)
    pl.semaphore_wait(barrier, 3)
    x_copy.wait()
    m_copy.wait()

    steps = [[], []]
    for h in range(hops):
        for b in range(2):
            for way in range(2):
                if h < hops - 1 or b == way:
                    steps[way].append((h, b))
    n_step = len(steps[0])

    def slot_of(way, h):
        return h if way == 0 else (n_chip - h) % n_chip

    def ring_x(way, j):
        h, b = steps[way][j]
        rows = pl.ds(b * half, half)
        return remote(xb.at[slot_of(way, h), 0, rows], xb.at[slot_of(way, h + 1), 0, rows],
                      ag_s.at[way, j], ag_r.at[way, j], left if way else right)

    def ring_meta(way, h):
        return remote(metab.at[slot_of(way, h), 0], metab.at[slot_of(way, h + 1), 0],
                      mt_s.at[way, h], mt_r.at[way, h], left if way else right)

    def pair_x(o, b):
        rows = pl.ds(b * half, half)
        return remote(xb.at[o, 0, rows], xb.at[o, 1, rows], pd_s.at[o, b], pd_r.at[o, b], partner)

    def pair_meta(o):
        return remote(metab.at[o, 0], metab.at[o, 1], pm_s.at[o], pm_r.at[o], partner)

    meta_hops = (hops, hops - 1)

    tri_r = lax.broadcasted_iota(jnp.int32, (LANES, LANES), 0)
    tri_c = lax.broadcasted_iota(jnp.int32, (LANES, LANES), 1)
    before = jnp.logical_and(tri_r < tri_c, (tri_r >= tok) == (tri_c >= tok))
    tri = jnp.where(before, 1.0, 0.0).astype(bf16)
    lane8 = lax.broadcasted_iota(jnp.int32, (8, LANES), 1)
    row8 = lax.broadcasted_iota(jnp.int32, (8, LANES), 0)
    slot_row = lax.broadcasted_iota(jnp.int32, (chip_cap, LANES), 0).astype(f32)

    def route(o):
        m0, m1 = metab[o, 0], metab[o, 1]
        low = lane8 < tok
        ids = jnp.where(low, m0, pltpu.roll(m1, tok, 1))
        gates = jnp.where(low, pltpu.roll(m0, tok, 1), m1)
        mask = jnp.zeros((8, LANES), f32)
        gate_rows = []
        for e in range(n_exp):
            hit = ids == (me * n_exp + e).astype(f32)
            row = jnp.sum(jnp.where(hit, 1.0, 0.0), axis=0, keepdims=True)
            mask = jnp.where(row8 == e, row, mask)
            gate_rows.append(jnp.sum(jnp.where(hit, gates, 0.0), axis=0, keepdims=True))
        pos = jnp.dot(mask.astype(bf16), tri, preferred_element_type=f32)
        pos = jnp.where(mask > 0.5, pos + jnp.where(low, 0.0, float(cap)), -1.0)
        pick = [jnp.where(slot_row == pos[e:e + 1, :], 1.0, 0.0) for e in range(n_exp)]
        pick_all = jnp.concatenate(pick, axis=0).astype(bf16)
        for n in range(d_model // COLS):
            cols = pl.ds(n * COLS, COLS)
            rows_x = jnp.concatenate([xb[o, 0, :, cols], xb[o, 1, :, cols]], axis=0)
            got = jnp.dot(pick_all, rows_x, preferred_element_type=f32).astype(bf16)
            for e in range(n_exp):
                xg[e, pl.ds(o * chip_cap, chip_cap), cols] = got[e * chip_cap:(e + 1) * chip_cap]
        weighted = [pick[e] * gate_rows[e] for e in range(n_exp)]
        weighted.append(jnp.zeros((COLS - slots, LANES), f32))
        rest = jnp.transpose(jnp.concatenate(weighted, axis=0))
        for part in range(3):
            piece = rest.astype(bf16)
            cmat[o, pl.ds(part * LANES, LANES), :] = piece
            rest = rest - piece.astype(f32)

    for way in range(2):
        ring_meta(way, 0).start()
    for j in range(2):
        for way in range(2):
            ring_x(way, j).start()
    pair_meta(0).start()
    for b in range(2):
        pair_x(0, b).start()

    def routed(o):
        pair_meta(o).wait_recv()
        for b in range(2):
            pair_x(o, b).wait_recv()
        route(o)

    for j in range(n_step):
        h = steps[0][j][0]
        if steps[0][j][1] == 0:
            for way in range(2):
                if h < meta_hops[way]:
                    ring_meta(way, h).wait_recv()
                    if h + 1 < meta_hops[way]:
                        ring_meta(way, h + 1).start()
                    pair_meta(slot_of(way, h + 1)).start()
        for way in range(2):
            ring_x(way, j).wait_recv()
            nxt = (steps[way][j][0] + 1, steps[way][j][1])
            if nxt in steps[way]:
                ring_x(way, steps[way].index(nxt)).start()
            pair_x(slot_of(way, h + 1), steps[way][j][1]).start()
        if j == 0:
            routed(0)
        elif j % 2 == 0 and h >= 1:
            routed(slot_of(0, h))
            routed(slot_of(1, h))
    routed(hops)

    def up_expert(e, carry):
        up_copy(e).wait()

        def up_cols(start, width):
            cols = pl.ds(start, width)
            raw = jnp.dot(xg[e], wup[e, :, cols], preferred_element_type=f32)
            hid[e, :, cols] = jax.nn.gelu(raw, approximate=True).astype(bf16)

        def up_step(n, inner):
            up_cols(pl.multiple_of(n * COLS, COLS), COLS)
            return inner

        lax.fori_loop(0, d_ff // COLS, up_step, 0)
        if d_ff % COLS:
            up_cols(d_ff - d_ff % COLS, d_ff % COLS)
        return carry

    lax.fori_loop(0, n_exp, up_expert, 0)

    for o in range(n_chip):
        ob[o, pl.ds(slots, COLS - slots), :] = jnp.zeros((COLS - slots, COLS), bf16)

    def pair_sum(c):
        slot = lax.rem(c, 2)
        return remote(psend.at[slot], precv.at[c], ps_s.at[c], ps_r.at[c], partner)

    def half_sum(way, c):
        rows = pl.ds(way * half, half)
        return remote(acc.at[c, hops, rows], rhalf.at[way, c], h_s.at[way, c], h_r.at[way, c], left if way else right)

    def full_sum(way, k, c):
        o = hops + k if way == 0 else hops - k
        return remote(acc.at[c, o], rfull.at[way, k - 1, c], f_s.at[way, k - 1, c], f_r.at[way, k - 1, c],
                      left if way else right)

    def down_chunk(c):
        slot = lax.rem(c, WD_SLOTS)
        wd_copy(c).wait()
        for e in range(n_exp):
            out = jnp.dot(hid[e], wd[slot, e], preferred_element_type=f32).astype(bf16)
            for o in range(n_chip):
                ob[o, pl.ds(e * chip_cap, chip_cap), :] = out[o * chip_cap:(o + 1) * chip_cap]

        @pl.when(c + WD_SLOTS < n_col)
        def _():
            wd_copy(c + WD_SLOTS).start()

        @pl.when(c >= 2)
        def _():
            pair_sum(c - 2).wait_send()

        for o in range(n_chip):
            got = jnp.dot(cmat[o], ob[o], preferred_element_type=f32)
            total = got[:LANES] + got[LANES:2 * LANES] + got[2 * LANES:]
            acc[c, o] = total[:tok]
            psend[lax.rem(c, 2), o] = total[tok:]
        pair_sum(c).start()

    def step(i, carry):
        @pl.when(i < n_col)
        def _():
            down_chunk(i)

        for k in range(1, hops + 1):
            c = i - k

            @pl.when(jnp.logical_and(c >= 0, c < n_col))
            def _():
                if k == 1:
                    for way in range(2):
                        half_sum(way, c).wait_recv()
                        o = hops + 1 if way == 0 else hops - 1
                        rows = pl.ds(way * half, half)
                        acc[c, o, rows, :] = acc[c, o, rows, :] + rhalf[way, c]
                        full_sum(way, 1, c).start()
                elif k < hops:
                    for way in range(2):
                        full_sum(way, k - 1, c).wait_recv()
                        o = hops + k if way == 0 else hops - k
                        acc[c, o] = acc[c, o] + rfull[way, k - 2, c]
                        full_sum(way, k, c).start()
                else:
                    total = acc[c, 0]
                    for way in range(2):
                        full_sum(way, hops - 1, c).wait_recv()
                        total = total + rfull[way, hops - 2, c]
                    cols = pl.ds(pl.multiple_of(c * COLS, COLS), COLS)
                    y_ref[:, cols] = total.astype(bf16)

        @pl.when(i < n_col)
        def _():
            pair_sum(i).wait_recv()
            for o in range(n_chip):
                acc[i, o] = acc[i, o] + precv[i, o]
            for way in range(2):
                half_sum(way, i).start()
        return carry

    lax.fori_loop(0, n_col + hops, step, 0)

    for way in range(2):
        for j in range(n_step):
            ring_x(way, j).wait_send()
        for h in range(meta_hops[way]):
            ring_meta(way, h).wait_send()
    for o in range(n_chip):
        pair_meta(o).wait_send()
        for b in range(2):
            pair_x(o, b).wait_send()

    def drain(c, carry):
        for way in range(2):
            half_sum(way, c).wait_send()
            for k in range(1, hops):
                full_sum(way, k, c).wait_send()

        @pl.when(c >= n_col - 2)
        def _():
            pair_sum(c).wait_send()
        return carry

    lax.fori_loop(0, n_col, drain, 0)


def solution(mesh):
    group = mesh.shape['expert']
    n_chip = group // 2
    hops = n_chip // 2

    def local_moe(x_loc, idx_loc, gate_loc, up_loc, down_loc):
        tok, d_model = x_loc.shape
        top_k = idx_loc.shape[1]
        n_exp, _, d_ff = up_loc.shape
        total_exp = n_exp * group
        cap = min(4, total_exp // top_k) * tok * top_k // total_exp
        n_col = d_model // COLS
        bf16, f32 = jnp.bfloat16, jnp.float32
        ids = jnp.pad(idx_loc.T.astype(f32), ((0, 8 - top_k), (0, 0)), constant_values=-1.0)
        gates = jnp.pad(gate_loc.T, ((0, 8 - top_k), (0, 0)))
        meta = jnp.concatenate([ids, gates], axis=1)
        dma = pltpu.SemaphoreType.DMA
        any_spec = pl.BlockSpec(memory_space=pl.ANY)
        n_step = 2 * hops - 1
        return pl.pallas_call(
            functools.partial(moe_kernel, group, cap),
            out_shape=jax.ShapeDtypeStruct((tok, d_model), bf16),
            in_specs=[any_spec] * 4,
            out_specs=pl.BlockSpec(memory_space=pltpu.VMEM),
            scratch_shapes=[
                pltpu.VMEM((n_exp, d_model, d_ff), bf16),
                pltpu.VMEM((WD_SLOTS, n_exp, d_ff, COLS), bf16),
                pltpu.VMEM((n_chip, 2, tok, d_model), bf16),
                pltpu.VMEM((n_chip, 2, 8, LANES), f32),
                pltpu.VMEM((n_exp, n_chip * 2 * cap, d_model), bf16),
                pltpu.VMEM((n_exp, n_chip * 2 * cap, d_ff), bf16),
                pltpu.VMEM((n_chip, 3 * LANES, COLS), bf16),
                pltpu.VMEM((n_chip, COLS, COLS), bf16),
                pltpu.VMEM((n_col, n_chip, tok, COLS), f32),
                pltpu.VMEM((2, n_chip, tok, COLS), f32),
                pltpu.VMEM((n_col, n_chip, tok, COLS), f32),
                pltpu.VMEM((2, n_col, tok // 2, COLS), f32),
                pltpu.VMEM((2, hops - 1, n_col, tok, COLS), f32),
                dma((2,)), dma((n_exp,)), dma((WD_SLOTS,)),
                dma((2, n_step)), dma((2, n_step)), dma((2, hops)), dma((2, hops)),
                dma((n_chip, 2)), dma((n_chip, 2)), dma((n_chip,)), dma((n_chip,)),
                dma((n_col,)), dma((n_col,)), dma((2, n_col)), dma((2, n_col)),
                dma((2, hops - 1, n_col)), dma((2, hops - 1, n_col)),
            ],
            compiler_params=pltpu.CompilerParams(
                collective_id=0, has_side_effects=True, vmem_limit_bytes=67043328),
        )(x_loc, meta, up_loc, down_loc)

    tok_spec = P(('data', 'expert'), None)
    w_spec = P('expert', None, None)
    return jax.shard_map(local_moe, mesh=mesh, in_specs=(tok_spec, tok_spec, tok_spec, w_spec, w_spec), out_specs=tok_spec, check_vma=False)
```

```python
import functools

import jax
import jax.numpy as jnp
from jax import lax
from jax.experimental import pallas as pl
from jax.experimental.pallas import tpu as pltpu
from jax.sharding import PartitionSpec as P

MESH = pl.DeviceIdType.MESH
COLS = 256
LANES = 128
WD_SLOTS = 3


def moe_kernel(group, cap, x_hbm, ids_ref, gate_ref, up_hbm, down_hbm, y_ref,
               wup, wd, xb, metab, xg, hid, cmat, ob, acc, psend, precv, rhalf, rfull,
               loc_sem, up_sem, wd_sem, ag_s, ag_r, mt_s, mt_r, pd_s, pd_r, pm_s, pm_r,
               ps_s, ps_r, h_s, h_r, f_s, f_r):
    n_chip = group // 2
    hops = n_chip // 2
    n_exp, d_model, d_ff = wup.shape
    tok = xb.shape[2]
    half = tok // 2
    chip_cap = 2 * cap
    slots = n_exp * chip_cap
    n_col = d_model // COLS
    f32, bf16 = jnp.float32, jnp.bfloat16

    me = lax.axis_index('expert')
    chip, core = me // 2, me % 2
    right = lax.rem(chip + 1, n_chip) * 2 + core
    left = lax.rem(chip + n_chip - 1, n_chip) * 2 + core
    partner = chip * 2 + 1 - core

    def remote(src, dst, send_sem, recv_sem, dev):
        return pltpu.make_async_remote_copy(src_ref=src, dst_ref=dst, send_sem=send_sem, recv_sem=recv_sem,
                                            device_id={'expert': dev}, device_id_type=MESH)

    x_copy = pltpu.make_async_copy(x_hbm, xb.at[0, 0], loc_sem)
    x_copy.start()
    top_k = ids_ref.shape[0]
    metab[0, 0] = jnp.full(metab.shape[2:], -1.0, f32)
    metab[0, 0, pl.ds(0, top_k), pl.ds(0, tok)] = ids_ref[...].astype(f32)
    metab[0, 0, pl.ds(8, top_k), pl.ds(0, tok)] = gate_ref[...]

    def up_copy(e):
        return pltpu.make_async_copy(up_hbm.at[e], wup.at[e], up_sem.at[e])

    def wd_copy(c):
        slot = lax.rem(c, WD_SLOTS)
        cols = pl.ds(pl.multiple_of(c * COLS, COLS), COLS)
        return pltpu.make_async_copy(down_hbm.at[:, :, cols], wd.at[slot], wd_sem.at[slot])

    for e in range(n_exp):
        up_copy(e).start()
    for c in range(min(WD_SLOTS, n_col)):
        wd_copy(jnp.int32(c)).start()

    barrier = pltpu.get_barrier_semaphore()
    for dev in (right, left, partner):
        pl.semaphore_signal(barrier, inc=1, device_id={'expert': dev}, device_id_type=MESH)
    pl.semaphore_wait(barrier, 3)
    x_copy.wait()

    steps = [[], []]
    for h in range(hops):
        for b in range(2):
            for way in range(2):
                if h < hops - 1 or b == way:
                    steps[way].append((h, b))
    n_step = len(steps[0])

    def slot_of(way, h):
        return h if way == 0 else (n_chip - h) % n_chip

    def ring_x(way, j):
        h, b = steps[way][j]
        rows = pl.ds(b * half, half)
        return remote(xb.at[slot_of(way, h), 0, rows], xb.at[slot_of(way, h + 1), 0, rows],
                      ag_s.at[way, j], ag_r.at[way, j], left if way else right)

    def ring_meta(way, h):
        return remote(metab.at[slot_of(way, h), 0], metab.at[slot_of(way, h + 1), 0],
                      mt_s.at[way, h], mt_r.at[way, h], left if way else right)

    def pair_x(o, b):
        rows = pl.ds(b * half, half)
        return remote(xb.at[o, 0, rows], xb.at[o, 1, rows], pd_s.at[o, b], pd_r.at[o, b], partner)

    def pair_meta(o):
        return remote(metab.at[o, 0], metab.at[o, 1], pm_s.at[o], pm_r.at[o], partner)

    meta_hops = (hops, hops - 1)

    order = [0]
    for h in range(1, hops):
        order += [h, n_chip - h]
    order.append(hops)
    place = {o: p for p, o in enumerate(order)}
    bounds = [0, 3, 5, n_chip]

    tri_r = lax.broadcasted_iota(jnp.int32, (LANES, LANES), 0)
    tri_c = lax.broadcasted_iota(jnp.int32, (LANES, LANES), 1)
    before = jnp.logical_and(tri_r < tri_c, (tri_r >= tok) == (tri_c >= tok))
    tri = jnp.where(before, 1.0, 0.0).astype(bf16)
    lane8 = lax.broadcasted_iota(jnp.int32, (8, LANES), 1)
    row8 = lax.broadcasted_iota(jnp.int32, (8, LANES), 0)
    slot_row = lax.broadcasted_iota(jnp.int32, (chip_cap, LANES), 0).astype(f32)

    def route(o):
        m0, m1 = metab[o, 0], metab[o, 1]
        low = lane8 < tok
        ids = jnp.where(low, m0[:8], pltpu.roll(m1[:8], tok, 1))
        gates = jnp.where(low, m0[8:], pltpu.roll(m1[8:], tok, 1))
        mask = jnp.zeros((8, LANES), f32)
        gate_rows = []
        for e in range(n_exp):
            hit = ids == (me * n_exp + e).astype(f32)
            row = jnp.sum(jnp.where(hit, 1.0, 0.0), axis=0, keepdims=True)
            mask = jnp.where(row8 == e, row, mask)
            gate_rows.append(jnp.sum(jnp.where(hit, gates, 0.0), axis=0, keepdims=True))
        pos = jnp.dot(mask.astype(bf16), tri, preferred_element_type=f32)
        pos = jnp.where(mask > 0.5, pos + jnp.where(low, 0.0, float(cap)), -1.0)
        pick = [jnp.where(slot_row == pos[e:e + 1, :], 1.0, 0.0) for e in range(n_exp)]
        pick_all = jnp.concatenate(pick, axis=0).astype(bf16)
        for n in range(d_model // COLS):
            cols = pl.ds(n * COLS, COLS)
            rows_x = jnp.concatenate([xb[o, 0, :, cols], xb[o, 1, :, cols]], axis=0)
            got = jnp.dot(pick_all, rows_x, preferred_element_type=f32).astype(bf16)
            for e in range(n_exp):
                xg[e, pl.ds(place[o] * chip_cap, chip_cap), cols] = got[e * chip_cap:(e + 1) * chip_cap]
        weighted = [pick[e] * gate_rows[e] for e in range(n_exp)]
        weighted.append(jnp.zeros((COLS - slots, LANES), f32))
        rest = jnp.transpose(jnp.concatenate(weighted, axis=0))
        for part in range(3):
            piece = rest.astype(bf16)
            cmat[o, pl.ds(part * LANES, LANES), :] = piece
            rest = rest - piece.astype(f32)

    for way in range(2):
        ring_meta(way, 0).start()
    for j in range(2):
        for way in range(2):
            ring_x(way, j).start()
    pair_meta(0).start()
    for b in range(2):
        pair_x(0, b).start()

    def routed(o):
        pair_meta(o).wait_recv()
        for b in range(2):
            pair_x(o, b).wait_recv()
        route(o)

    def gather_step(j):
        h = steps[0][j][0]
        if steps[0][j][1] == 0:
            for way in range(2):
                if h < meta_hops[way]:
                    ring_meta(way, h).wait_recv()
                    if h + 1 < meta_hops[way]:
                        ring_meta(way, h + 1).start()
                    pair_meta(slot_of(way, h + 1)).start()
        for way in range(2):
            ring_x(way, j).wait_recv()
            nxt = (steps[way][j][0] + 1, steps[way][j][1])
            if nxt in steps[way]:
                ring_x(way, steps[way].index(nxt)).start()
            pair_x(slot_of(way, h + 1), steps[way][j][1]).start()

    def up_rows(phase, first, last):
        rows = pl.ds(bounds[phase] * chip_cap, (bounds[phase + 1] - bounds[phase]) * chip_cap)

        def expert(e, carry):
            if phase == 0:
                up_copy(e).wait()
            for start in range(0, d_ff, COLS):
                cols = pl.ds(start, min(COLS, d_ff - start))
                raw = jnp.dot(xg[e, rows, :], wup[e, :, cols], preferred_element_type=f32)
                hid[e, rows, cols] = jax.nn.gelu(raw, approximate=True).astype(bf16)
            return carry

        lax.fori_loop(first, last, expert, 0)

    routed(0)
    gather_step(0)
    gather_step(1)
    routed(1)
    routed(n_chip - 1)
    gather_step(2)
    up_rows(0, 0, n_exp // 2)
    gather_step(3)
    up_rows(0, n_exp // 2, n_exp)
    gather_step(4)
    routed(2)
    routed(n_chip - 2)
    up_rows(1, 0, 1)
    gather_step(5)
    up_rows(1, 1, n_exp - 1)
    gather_step(6)
    up_rows(1, n_exp - 1, n_exp)
    routed(3)
    routed(n_chip - 3)
    routed(hops)
    up_rows(2, 0, n_exp)

    for o in range(n_chip):
        ob[o, pl.ds(slots, COLS - slots), :] = jnp.zeros((COLS - slots, COLS), bf16)

    def pair_sum(c, k):
        slot = lax.rem(c, 2)
        part = pl.ds(k, 1 if k == 0 else n_chip - 1)
        return remote(psend.at[slot, part], precv.at[c, part], ps_s.at[c, k], ps_r.at[c, k], partner)

    far_first = order[::-1]

    def half_sum(way, c):
        rows = pl.ds(way * half, half)
        return remote(acc.at[c, hops, rows], rhalf.at[way, c], h_s.at[way, c], h_r.at[way, c], left if way else right)

    def full_sum(way, k, c):
        o = hops + k if way == 0 else hops - k
        return remote(acc.at[c, o], rfull.at[way, k - 1, c], f_s.at[way, k - 1, c], f_r.at[way, k - 1, c],
                      left if way else right)

    def down_chunk(c):
        slot = lax.rem(c, WD_SLOTS)
        wd_copy(c).wait()
        for e in range(n_exp):
            out = jnp.dot(hid[e], wd[slot, e], preferred_element_type=f32).astype(bf16)
            for o in range(n_chip):
                ob[o, pl.ds(e * chip_cap, chip_cap), :] = out[place[o] * chip_cap:(place[o] + 1) * chip_cap]

        @pl.when(c + WD_SLOTS < n_col)
        def _():
            wd_copy(c + WD_SLOTS).start()

        @pl.when(c >= 2)
        def _():
            for k in range(2):
                pair_sum(c - 2, k).wait_send()

        for p, o in enumerate(far_first):
            got = jnp.dot(cmat[o], ob[o], preferred_element_type=f32)
            total = got[:LANES] + got[LANES:2 * LANES] + got[2 * LANES:]
            acc[c, o] = total[:tok]
            psend[lax.rem(c, 2), p] = total[tok:]
            if p == 0:
                pair_sum(c, 0).start()
        pair_sum(c, 1).start()

    def step(i, carry):
        @pl.when(i < n_col)
        def _():
            down_chunk(i)

        for k in range(1, hops + 1):
            c = i - k

            @pl.when(jnp.logical_and(c >= 0, c < n_col))
            def _():
                if k == 1:
                    for way in range(2):
                        half_sum(way, c).wait_recv()
                        o = hops + 1 if way == 0 else hops - 1
                        rows = pl.ds(way * half, half)
                        acc[c, o, rows, :] = acc[c, o, rows, :] + rhalf[way, c]
                        full_sum(way, 1, c).start()
                elif k < hops:
                    for way in range(2):
                        full_sum(way, k - 1, c).wait_recv()
                        o = hops + k if way == 0 else hops - k
                        acc[c, o] = acc[c, o] + rfull[way, k - 2, c]
                        full_sum(way, k, c).start()
                else:
                    total = acc[c, 0]
                    for way in range(2):
                        full_sum(way, hops - 1, c).wait_recv()
                        total = total + rfull[way, hops - 2, c]
                    cols = pl.ds(pl.multiple_of(c * COLS, COLS), COLS)
                    y_ref[:, cols] = total.astype(bf16)

        @pl.when(i < n_col)
        def _():
            pair_sum(i, 0).wait_recv()
            acc[i, hops] = acc[i, hops] + precv[i, 0]
            for way in range(2):
                half_sum(way, i).start()
            pair_sum(i, 1).wait_recv()
            for p, o in enumerate(far_first[1:], 1):
                acc[i, o] = acc[i, o] + precv[i, p]
        return carry

    lax.fori_loop(0, n_col + hops, step, 0)

    for way in range(2):
        for j in range(n_step):
            ring_x(way, j).wait_send()
        for h in range(meta_hops[way]):
            ring_meta(way, h).wait_send()
    for o in range(n_chip):
        pair_meta(o).wait_send()
        for b in range(2):
            pair_x(o, b).wait_send()

    def drain(c, carry):
        for way in range(2):
            half_sum(way, c).wait_send()
            for k in range(1, hops):
                full_sum(way, k, c).wait_send()

        @pl.when(c >= n_col - 2)
        def _():
            for k in range(2):
                pair_sum(c, k).wait_send()
        return carry

    lax.fori_loop(0, n_col, drain, 0)


def solution(mesh):
    group = mesh.shape['expert']
    n_chip = group // 2
    hops = n_chip // 2

    def local_moe(x_loc, idx_loc, gate_loc, up_loc, down_loc):
        tok, d_model = x_loc.shape
        top_k = idx_loc.shape[1]
        n_exp, _, d_ff = up_loc.shape
        total_exp = n_exp * group
        cap = min(4, total_exp // top_k) * tok * top_k // total_exp
        n_col = d_model // COLS
        bf16, f32 = jnp.bfloat16, jnp.float32
        dma = pltpu.SemaphoreType.DMA
        any_spec = pl.BlockSpec(memory_space=pl.ANY)
        vmem_spec = pl.BlockSpec(memory_space=pltpu.VMEM)
        n_step = 2 * hops - 1
        return pl.pallas_call(
            functools.partial(moe_kernel, group, cap),
            out_shape=jax.ShapeDtypeStruct((tok, d_model), bf16),
            in_specs=[any_spec, vmem_spec, vmem_spec, any_spec, any_spec],
            out_specs=vmem_spec,
            scratch_shapes=[
                pltpu.VMEM((n_exp, d_model, d_ff), bf16),
                pltpu.VMEM((WD_SLOTS, n_exp, d_ff, COLS), bf16),
                pltpu.VMEM((n_chip, 2, tok, d_model), bf16),
                pltpu.VMEM((n_chip, 2, 16, LANES), f32),
                pltpu.VMEM((n_exp, n_chip * 2 * cap, d_model), bf16),
                pltpu.VMEM((n_exp, n_chip * 2 * cap, d_ff), bf16),
                pltpu.VMEM((n_chip, 3 * LANES, COLS), bf16),
                pltpu.VMEM((n_chip, COLS, COLS), bf16),
                pltpu.VMEM((n_col, n_chip, tok, COLS), f32),
                pltpu.VMEM((2, n_chip, tok, COLS), f32),
                pltpu.VMEM((n_col, n_chip, tok, COLS), f32),
                pltpu.VMEM((2, n_col, tok // 2, COLS), f32),
                pltpu.VMEM((2, hops - 1, n_col, tok, COLS), f32),
                dma, dma((n_exp,)), dma((WD_SLOTS,)),
                dma((2, n_step)), dma((2, n_step)), dma((2, hops)), dma((2, hops)),
                dma((n_chip, 2)), dma((n_chip, 2)), dma((n_chip,)), dma((n_chip,)),
                dma((n_col, 2)), dma((n_col, 2)), dma((2, n_col)), dma((2, n_col)),
                dma((2, hops - 1, n_col)), dma((2, hops - 1, n_col)),
            ],
            compiler_params=pltpu.CompilerParams(
                collective_id=0, has_side_effects=True, vmem_limit_bytes=67043328),
        )(x_loc, idx_loc.T, gate_loc.T, up_loc, down_loc)

    tok_spec = P(('data', 'expert'), None)
    w_spec = P('expert', None, None)
    return jax.shard_map(local_moe, mesh=mesh, in_specs=(tok_spec, tok_spec, tok_spec, w_spec, w_spec), out_specs=tok_spec, check_vma=False)
```

```python
import functools

import jax
import jax.numpy as jnp
from jax import lax
from jax.experimental import pallas as pl
from jax.experimental.pallas import tpu as pltpu
from jax.sharding import PartitionSpec as P

MESH = pl.DeviceIdType.MESH
COLS = 256
LANES = 128
WD_SLOTS = 3


def moe_kernel(group, cap, x_hbm, ids_ref, gate_ref, up_hbm, down_hbm, y_ref,
               wup, wd, xb, metab, xg, hid, cmat, ob, acc, psend, precv, rhalf, rfull,
               loc_sem, up_sem, wd_sem, ag_s, ag_r, mt_s, mt_r, pd_s, pd_r, pm_s, pm_r,
               ps_s, ps_r, h_s, h_r, f_s, f_r):
    n_chip = group // 2
    hops = n_chip // 2
    n_exp, d_model, d_ff = wup.shape
    tok = xb.shape[2]
    half = tok // 2
    chip_cap = 2 * cap
    slots = n_exp * chip_cap
    n_col = d_model // COLS
    f32, bf16 = jnp.float32, jnp.bfloat16

    me = lax.axis_index('expert')
    chip, core = me // 2, me % 2
    right = lax.rem(chip + 1, n_chip) * 2 + core
    left = lax.rem(chip + n_chip - 1, n_chip) * 2 + core
    partner = chip * 2 + 1 - core

    def remote(src, dst, send_sem, recv_sem, dev):
        return pltpu.make_async_remote_copy(src_ref=src, dst_ref=dst, send_sem=send_sem, recv_sem=recv_sem,
                                            device_id={'expert': dev}, device_id_type=MESH)

    x_copy = pltpu.make_async_copy(x_hbm, xb.at[0, 0], loc_sem)
    x_copy.start()
    top_k = ids_ref.shape[0]
    metab[0, 0] = jnp.full(metab.shape[2:], -1.0, f32)
    metab[0, 0, pl.ds(0, top_k), pl.ds(0, tok)] = ids_ref[...].astype(f32)
    metab[0, 0, pl.ds(8, top_k), pl.ds(0, tok)] = gate_ref[...]

    def up_copy(e):
        return pltpu.make_async_copy(up_hbm.at[e], wup.at[e], up_sem.at[e])

    def wd_copy(c):
        slot = lax.rem(c, WD_SLOTS)
        cols = pl.ds(pl.multiple_of(c * COLS, COLS), COLS)
        return pltpu.make_async_copy(down_hbm.at[:, :, cols], wd.at[slot], wd_sem.at[slot])

    for e in range(n_exp):
        up_copy(e).start()
    for c in range(min(WD_SLOTS, n_col)):
        wd_copy(jnp.int32(c)).start()

    barrier = pltpu.get_barrier_semaphore()
    for dev in (right, left, partner):
        pl.semaphore_signal(barrier, inc=1, device_id={'expert': dev}, device_id_type=MESH)
    pl.semaphore_wait(barrier, 3)
    x_copy.wait()

    steps = [[], []]
    for h in range(hops):
        for b in range(2):
            for way in range(2):
                if h < hops - 1 or b == way:
                    steps[way].append((h, b))
    n_step = len(steps[0])

    def slot_of(way, h):
        return h if way == 0 else (n_chip - h) % n_chip

    def ring_x(way, j):
        h, b = steps[way][j]
        rows = pl.ds(b * half, half)
        return remote(xb.at[slot_of(way, h), 0, rows], xb.at[slot_of(way, h + 1), 0, rows],
                      ag_s.at[way, j], ag_r.at[way, j], left if way else right)

    def ring_meta(way, h):
        return remote(metab.at[slot_of(way, h), 0], metab.at[slot_of(way, h + 1), 0],
                      mt_s.at[way, h], mt_r.at[way, h], left if way else right)

    def pair_x(o, b):
        rows = pl.ds(b * half, half)
        return remote(xb.at[o, 0, rows], xb.at[o, 1, rows], pd_s.at[o, b], pd_r.at[o, b], partner)

    def pair_meta(o):
        return remote(metab.at[o, 0], metab.at[o, 1], pm_s.at[o], pm_r.at[o], partner)

    meta_hops = (hops, hops - 1)

    order = [0]
    for h in range(1, hops):
        order += [h, n_chip - h]
    order.append(hops)
    place = {o: p for p, o in enumerate(order)}
    bounds = [0, 3, 5, n_chip]

    tri_r = lax.broadcasted_iota(jnp.int32, (LANES, LANES), 0)
    tri_c = lax.broadcasted_iota(jnp.int32, (LANES, LANES), 1)
    before = jnp.logical_and(tri_r < tri_c, (tri_r >= tok) == (tri_c >= tok))
    tri = jnp.where(before, 1.0, 0.0).astype(bf16)
    lane8 = lax.broadcasted_iota(jnp.int32, (8, LANES), 1)
    row8 = lax.broadcasted_iota(jnp.int32, (8, LANES), 0)
    slot_row = lax.broadcasted_iota(jnp.int32, (chip_cap, LANES), 0).astype(f32)

    def route(o):
        m0, m1 = metab[o, 0], metab[o, 1]
        low = lane8 < tok
        ids = jnp.where(low, m0[:8], pltpu.roll(m1[:8], tok, 1))
        gates = jnp.where(low, m0[8:], pltpu.roll(m1[8:], tok, 1))
        mask = jnp.zeros((8, LANES), f32)
        gate_rows = []
        for e in range(n_exp):
            hit = ids == (me * n_exp + e).astype(f32)
            row = jnp.sum(jnp.where(hit, 1.0, 0.0), axis=0, keepdims=True)
            mask = jnp.where(row8 == e, row, mask)
            gate_rows.append(jnp.sum(jnp.where(hit, gates, 0.0), axis=0, keepdims=True))
        pos = jnp.dot(mask.astype(bf16), tri, preferred_element_type=f32)
        pos = jnp.where(mask > 0.5, pos + jnp.where(low, 0.0, float(cap)), -1.0)
        pick = [jnp.where(slot_row == pos[e:e + 1, :], 1.0, 0.0) for e in range(n_exp)]
        pick_all = jnp.concatenate(pick, axis=0).astype(bf16)
        for n in range(d_model // COLS):
            cols = pl.ds(n * COLS, COLS)
            rows_x = jnp.concatenate([xb[o, 0, :, cols], xb[o, 1, :, cols]], axis=0)
            got = jnp.dot(pick_all, rows_x, preferred_element_type=f32).astype(bf16)
            for e in range(n_exp):
                xg[e, pl.ds(place[o] * chip_cap, chip_cap), cols] = got[e * chip_cap:(e + 1) * chip_cap]
        weighted = [pick[e] * gate_rows[e] for e in range(n_exp)]
        weighted.append(jnp.zeros((COLS - slots, LANES), f32))
        rest = jnp.transpose(jnp.concatenate(weighted, axis=0))
        for part in range(3):
            piece = rest.astype(bf16)
            cmat[o, pl.ds(part * LANES, LANES), :] = piece
            rest = rest - piece.astype(f32)

    for way in range(2):
        ring_meta(way, 0).start()
    for j in range(2):
        for way in range(2):
            ring_x(way, j).start()
    pair_meta(0).start()
    for b in range(2):
        pair_x(0, b).start()

    def routed(o):
        pair_meta(o).wait_recv()
        for b in range(2):
            pair_x(o, b).wait_recv()
        route(o)

    def gather_step(j):
        h = steps[0][j][0]
        if steps[0][j][1] == 0:
            for way in range(2):
                if h < meta_hops[way]:
                    ring_meta(way, h).wait_recv()
                    if h + 1 < meta_hops[way]:
                        ring_meta(way, h + 1).start()
                    pair_meta(slot_of(way, h + 1)).start()
        for way in range(2):
            ring_x(way, j).wait_recv()
            nxt = (steps[way][j][0] + 1, steps[way][j][1])
            if nxt in steps[way]:
                ring_x(way, steps[way].index(nxt)).start()
            pair_x(slot_of(way, h + 1), steps[way][j][1]).start()

    def up_rows(phase, first, last):
        rows = pl.ds(bounds[phase] * chip_cap, (bounds[phase + 1] - bounds[phase]) * chip_cap)

        def expert(e, carry):
            if phase == 0:
                up_copy(e).wait()
            for start in range(0, d_ff, COLS):
                cols = pl.ds(start, min(COLS, d_ff - start))
                raw = jnp.dot(xg[e, rows, :], wup[e, :, cols], preferred_element_type=f32)
                hid[e, rows, cols] = jax.nn.gelu(raw, approximate=True).astype(bf16)
            return carry

        lax.fori_loop(first, last, expert, 0)

    routed(0)
    gather_step(0)
    gather_step(1)
    routed(1)
    routed(n_chip - 1)
    gather_step(2)
    up_rows(0, 0, n_exp // 2)
    gather_step(3)
    up_rows(0, n_exp // 2, n_exp)
    routed(2)
    routed(n_chip - 2)
    gather_step(4)
    up_rows(1, 0, n_exp // 2)
    gather_step(5)
    up_rows(1, n_exp // 2, n_exp)
    routed(3)
    routed(n_chip - 3)
    gather_step(6)
    routed(hops)
    up_rows(2, 0, n_exp)

    for o in range(n_chip):
        ob[o, pl.ds(slots, COLS - slots), :] = jnp.zeros((COLS - slots, COLS), bf16)

    def pair_sum(c, k):
        slot = lax.rem(c, 2)
        part = pl.ds(k, 1 if k == 0 else n_chip - 1)
        return remote(psend.at[slot, part], precv.at[c, part], ps_s.at[c, k], ps_r.at[c, k], partner)

    far_first = order[::-1]

    def half_sum(way, c):
        rows = pl.ds(way * half, half)
        return remote(acc.at[c, hops, rows], rhalf.at[way, c], h_s.at[way, c], h_r.at[way, c], left if way else right)

    def full_sum(way, k, c):
        o = hops + k if way == 0 else hops - k
        return remote(acc.at[c, o], rfull.at[way, k - 1, c], f_s.at[way, k - 1, c], f_r.at[way, k - 1, c],
                      left if way else right)

    def down_chunk(c):
        slot = lax.rem(c, WD_SLOTS)
        wd_copy(c).wait()
        for e in range(n_exp):
            out = jnp.dot(hid[e], wd[slot, e], preferred_element_type=f32).astype(bf16)
            for o in range(n_chip):
                ob[o, pl.ds(e * chip_cap, chip_cap), :] = out[place[o] * chip_cap:(place[o] + 1) * chip_cap]

        @pl.when(c + WD_SLOTS < n_col)
        def _():
            wd_copy(c + WD_SLOTS).start()

        @pl.when(c >= 2)
        def _():
            for k in range(2):
                pair_sum(c - 2, k).wait_send()

        for p, o in enumerate(far_first):
            got = jnp.dot(cmat[o], ob[o], preferred_element_type=f32)
            total = got[:LANES] + got[LANES:2 * LANES] + got[2 * LANES:]
            acc[c, o] = total[:tok]
            psend[lax.rem(c, 2), p] = total[tok:]
            if p == 0:
                pair_sum(c, 0).start()
        pair_sum(c, 1).start()

    def step(i, carry):
        @pl.when(i < n_col)
        def _():
            down_chunk(i)
            pair_sum(i, 0).wait_recv()
            acc[i, hops] = acc[i, hops] + precv[i, 0]
            for way in range(2):
                half_sum(way, i).start()
            pair_sum(i, 1).wait_recv()
            for p, o in enumerate(far_first[1:], 1):
                acc[i, o] = acc[i, o] + precv[i, p]

        for k in range(1, hops + 1):
            c = i - k if k < hops else i - hops - 1

            @pl.when(jnp.logical_and(c >= 0, c < n_col))
            def _():
                if k == 1:
                    for way in range(2):
                        half_sum(way, c).wait_recv()
                        o = hops + 1 if way == 0 else hops - 1
                        rows = pl.ds(way * half, half)
                        acc[c, o, rows, :] = acc[c, o, rows, :] + rhalf[way, c]
                        full_sum(way, 1, c).start()
                elif k < hops:
                    for way in range(2):
                        full_sum(way, k - 1, c).wait_recv()
                        o = hops + k if way == 0 else hops - k
                        acc[c, o] = acc[c, o] + rfull[way, k - 2, c]
                        full_sum(way, k, c).start()
                else:
                    total = acc[c, 0]
                    for way in range(2):
                        full_sum(way, hops - 1, c).wait_recv()
                        total = total + rfull[way, hops - 2, c]
                    cols = pl.ds(pl.multiple_of(c * COLS, COLS), COLS)
                    y_ref[:, cols] = total.astype(bf16)

        return carry

    lax.fori_loop(0, n_col + hops + 1, step, 0)

    for way in range(2):
        for j in range(n_step):
            ring_x(way, j).wait_send()
        for h in range(meta_hops[way]):
            ring_meta(way, h).wait_send()
    for o in range(n_chip):
        pair_meta(o).wait_send()
        for b in range(2):
            pair_x(o, b).wait_send()

    def drain(c, carry):
        for way in range(2):
            half_sum(way, c).wait_send()
            for k in range(1, hops):
                full_sum(way, k, c).wait_send()

        @pl.when(c >= n_col - 2)
        def _():
            for k in range(2):
                pair_sum(c, k).wait_send()
        return carry

    lax.fori_loop(0, n_col, drain, 0)


def solution(mesh):
    group = mesh.shape['expert']
    n_chip = group // 2
    hops = n_chip // 2

    def local_moe(x_loc, idx_loc, gate_loc, up_loc, down_loc):
        tok, d_model = x_loc.shape
        top_k = idx_loc.shape[1]
        n_exp, _, d_ff = up_loc.shape
        total_exp = n_exp * group
        cap = min(4, total_exp // top_k) * tok * top_k // total_exp
        n_col = d_model // COLS
        bf16, f32 = jnp.bfloat16, jnp.float32
        dma = pltpu.SemaphoreType.DMA
        any_spec = pl.BlockSpec(memory_space=pl.ANY)
        vmem_spec = pl.BlockSpec(memory_space=pltpu.VMEM)
        n_step = 2 * hops - 1
        return pl.pallas_call(
            functools.partial(moe_kernel, group, cap),
            out_shape=jax.ShapeDtypeStruct((tok, d_model), bf16),
            in_specs=[any_spec, vmem_spec, vmem_spec, any_spec, any_spec],
            out_specs=vmem_spec,
            scratch_shapes=[
                pltpu.VMEM((n_exp, d_model, d_ff), bf16),
                pltpu.VMEM((WD_SLOTS, n_exp, d_ff, COLS), bf16),
                pltpu.VMEM((n_chip, 2, tok, d_model), bf16),
                pltpu.VMEM((n_chip, 2, 16, LANES), f32),
                pltpu.VMEM((n_exp, n_chip * 2 * cap, d_model), bf16),
                pltpu.VMEM((n_exp, n_chip * 2 * cap, d_ff), bf16),
                pltpu.VMEM((n_chip, 3 * LANES, COLS), bf16),
                pltpu.VMEM((n_chip, COLS, COLS), bf16),
                pltpu.VMEM((n_col, n_chip, tok, COLS), f32),
                pltpu.VMEM((2, n_chip, tok, COLS), f32),
                pltpu.VMEM((n_col, n_chip, tok, COLS), f32),
                pltpu.VMEM((2, n_col, tok // 2, COLS), f32),
                pltpu.VMEM((2, hops - 1, n_col, tok, COLS), f32),
                dma, dma((n_exp,)), dma((WD_SLOTS,)),
                dma((2, n_step)), dma((2, n_step)), dma((2, hops)), dma((2, hops)),
                dma((n_chip, 2)), dma((n_chip, 2)), dma((n_chip,)), dma((n_chip,)),
                dma((n_col, 2)), dma((n_col, 2)), dma((2, n_col)), dma((2, n_col)),
                dma((2, hops - 1, n_col)), dma((2, hops - 1, n_col)),
            ],
            compiler_params=pltpu.CompilerParams(
                collective_id=0, has_side_effects=True, vmem_limit_bytes=67043328),
        )(x_loc, idx_loc.T, gate_loc.T, up_loc, down_loc)

    tok_spec = P(('data', 'expert'), None)
    w_spec = P('expert', None, None)
    return jax.shard_map(local_moe, mesh=mesh, in_specs=(tok_spec, tok_spec, tok_spec, w_spec, w_spec), out_specs=tok_spec, check_vma=False)
```

```python
import functools

import jax
import jax.numpy as jnp
from jax import lax
from jax.experimental import pallas as pl
from jax.experimental.pallas import tpu as pltpu
from jax.sharding import PartitionSpec as P

MESH = pl.DeviceIdType.MESH
COLS = 256
LANES = 128
WD_SLOTS = 3


def moe_kernel(group, cap, x_hbm, ids_ref, gate_ref, up_hbm, down_hbm, y_ref,
               wup, wd, xb, metab, xg, hid, cmat, ob, acc, psend, precv, rhalf, rfull,
               loc_sem, up_sem, wd_sem, ag_s, ag_r, mt_s, mt_r, pd_s, pd_r, pm_s, pm_r,
               ps_s, ps_r, h_s, h_r, f_s, f_r):
    n_chip = group // 2
    hops = n_chip // 2
    n_exp, d_model, d_ff = wup.shape
    tok = xb.shape[2]
    half = tok // 2
    chip_cap = 2 * cap
    slots = n_exp * chip_cap
    n_col = d_model // COLS
    f32, bf16 = jnp.float32, jnp.bfloat16

    me = lax.axis_index('expert')
    chip, core = me // 2, me % 2
    right = lax.rem(chip + 1, n_chip) * 2 + core
    left = lax.rem(chip + n_chip - 1, n_chip) * 2 + core
    partner = chip * 2 + 1 - core

    def remote(src, dst, send_sem, recv_sem, dev):
        return pltpu.make_async_remote_copy(src_ref=src, dst_ref=dst, send_sem=send_sem, recv_sem=recv_sem,
                                            device_id={'expert': dev}, device_id_type=MESH)

    x_copy = pltpu.make_async_copy(x_hbm, xb.at[0, 0], loc_sem)
    x_copy.start()
    top_k = ids_ref.shape[0]
    metab[0, 0] = jnp.full(metab.shape[2:], -1.0, f32)
    metab[0, 0, pl.ds(0, top_k), pl.ds(0, tok)] = ids_ref[...].astype(f32)
    metab[0, 0, pl.ds(8, top_k), pl.ds(0, tok)] = gate_ref[...]

    def up_copy(e):
        return pltpu.make_async_copy(up_hbm.at[e], wup.at[e], up_sem.at[e])

    def wd_copy(load):
        slot = lax.rem(load, WD_SLOTS)
        cols = pl.ds(pl.multiple_of(lax.rem(load, n_col) * COLS, COLS), COLS)
        return pltpu.make_async_copy(down_hbm.at[:, :, cols], wd.at[slot], wd_sem.at[slot])

    for e in range(n_exp):
        up_copy(e).start()
    for c in range(min(WD_SLOTS, n_col)):
        wd_copy(jnp.int32(c)).start()

    barrier = pltpu.get_barrier_semaphore()
    for dev in (right, left, partner):
        pl.semaphore_signal(barrier, inc=1, device_id={'expert': dev}, device_id_type=MESH)
    pl.semaphore_wait(barrier, 3)
    x_copy.wait()

    steps = [[], []]
    for h in range(hops):
        for b in range(2):
            for way in range(2):
                if h < hops - 1 or b == way:
                    steps[way].append((h, b))
    n_step = len(steps[0])

    def slot_of(way, h):
        return h if way == 0 else (n_chip - h) % n_chip

    def ring_x(way, j):
        h, b = steps[way][j]
        rows = pl.ds(b * half, half)
        return remote(xb.at[slot_of(way, h), 0, rows], xb.at[slot_of(way, h + 1), 0, rows],
                      ag_s.at[way, j], ag_r.at[way, j], left if way else right)

    def ring_meta(way, h):
        return remote(metab.at[slot_of(way, h), 0], metab.at[slot_of(way, h + 1), 0],
                      mt_s.at[way, h], mt_r.at[way, h], left if way else right)

    def pair_x(o, b):
        rows = pl.ds(b * half, half)
        return remote(xb.at[o, 0, rows], xb.at[o, 1, rows], pd_s.at[o, b], pd_r.at[o, b], partner)

    def pair_meta(o):
        return remote(metab.at[o, 0], metab.at[o, 1], pm_s.at[o], pm_r.at[o], partner)

    meta_hops = (hops, hops - 1)

    order = [0]
    for h in range(1, hops):
        order += [h, n_chip - h]
    order.append(hops)
    place = {o: p for p, o in enumerate(order)}
    bounds = [0, 3, 5, n_chip]

    tri_r = lax.broadcasted_iota(jnp.int32, (LANES, LANES), 0)
    tri_c = lax.broadcasted_iota(jnp.int32, (LANES, LANES), 1)
    before = jnp.logical_and(tri_r < tri_c, (tri_r >= tok) == (tri_c >= tok))
    tri = jnp.where(before, 1.0, 0.0).astype(bf16)
    lane8 = lax.broadcasted_iota(jnp.int32, (8, LANES), 1)
    row8 = lax.broadcasted_iota(jnp.int32, (8, LANES), 0)
    slot_row = lax.broadcasted_iota(jnp.int32, (chip_cap, LANES), 0).astype(f32)

    def route(o):
        m0, m1 = metab[o, 0], metab[o, 1]
        low = lane8 < tok
        ids = jnp.where(low, m0[:8], pltpu.roll(m1[:8], tok, 1))
        gates = jnp.where(low, m0[8:], pltpu.roll(m1[8:], tok, 1))
        mask = jnp.zeros((8, LANES), f32)
        gate_rows = []
        for e in range(n_exp):
            hit = ids == (me * n_exp + e).astype(f32)
            row = jnp.sum(jnp.where(hit, 1.0, 0.0), axis=0, keepdims=True)
            mask = jnp.where(row8 == e, row, mask)
            gate_rows.append(jnp.sum(jnp.where(hit, gates, 0.0), axis=0, keepdims=True))
        pos = jnp.dot(mask.astype(bf16), tri, preferred_element_type=f32)
        pos = jnp.where(mask > 0.5, pos + jnp.where(low, 0.0, float(cap)), -1.0)
        pick = [jnp.where(slot_row == pos[e:e + 1, :], 1.0, 0.0) for e in range(n_exp)]
        pick_all = jnp.concatenate(pick, axis=0).astype(bf16)
        for n in range(d_model // COLS):
            cols = pl.ds(n * COLS, COLS)
            rows_x = jnp.concatenate([xb[o, 0, :, cols], xb[o, 1, :, cols]], axis=0)
            got = jnp.dot(pick_all, rows_x, preferred_element_type=f32).astype(bf16)
            for e in range(n_exp):
                xg[e, pl.ds(place[o] * chip_cap, chip_cap), cols] = got[e * chip_cap:(e + 1) * chip_cap]
        weighted = [pick[e] * gate_rows[e] for e in range(n_exp)]
        weighted.append(jnp.zeros((COLS - slots, LANES), f32))
        rest = jnp.transpose(jnp.concatenate(weighted, axis=0))
        for part in range(3):
            piece = rest.astype(bf16)
            cmat[o, pl.ds(part * LANES, LANES), :] = piece
            rest = rest - piece.astype(f32)

    for way in range(2):
        ring_meta(way, 0).start()
    for j in range(2):
        for way in range(2):
            ring_x(way, j).start()
    pair_meta(0).start()
    for b in range(2):
        pair_x(0, b).start()

    def routed(o):
        pair_meta(o).wait_recv()
        for b in range(2):
            pair_x(o, b).wait_recv()
        route(o)

    def gather_step(j):
        h = steps[0][j][0]
        if steps[0][j][1] == 0:
            for way in range(2):
                if h < meta_hops[way]:
                    ring_meta(way, h).wait_recv()
                    if h + 1 < meta_hops[way]:
                        ring_meta(way, h + 1).start()
                    pair_meta(slot_of(way, h + 1)).start()
        for way in range(2):
            ring_x(way, j).wait_recv()
            nxt = (steps[way][j][0] + 1, steps[way][j][1])
            if nxt in steps[way]:
                ring_x(way, steps[way].index(nxt)).start()
            pair_x(slot_of(way, h + 1), steps[way][j][1]).start()

    def up_rows(phase, first, last):
        rows = pl.ds(bounds[phase] * chip_cap, (bounds[phase + 1] - bounds[phase]) * chip_cap)

        def expert(e, carry):
            if phase == 0:
                up_copy(e).wait()
            for start in range(0, d_ff, COLS):
                cols = pl.ds(start, min(COLS, d_ff - start))
                raw = jnp.dot(xg[e, rows, :], wup[e, :, cols], preferred_element_type=f32)
                hid[e, rows, cols] = jax.nn.gelu(raw, approximate=True).astype(bf16)
            return carry

        lax.fori_loop(first, last, expert, 0)

    routed(0)
    gather_step(0)
    gather_step(1)
    routed(1)
    routed(n_chip - 1)
    gather_step(2)
    up_rows(0, 0, n_exp // 2)
    gather_step(3)
    up_rows(0, n_exp // 2, n_exp)
    routed(2)
    routed(n_chip - 2)
    gather_step(4)
    up_rows(1, 0, n_exp // 2)
    gather_step(5)
    up_rows(1, n_exp // 2, n_exp)
    routed(3)
    routed(n_chip - 3)
    gather_step(6)
    routed(hops)
    up_rows(2, 0, n_exp)

    for o in range(n_chip):
        ob[o, pl.ds(slots, COLS - slots), :] = jnp.zeros((COLS - slots, COLS), bf16)

    far_first = order[::-1]
    n_last = n_chip - bounds[2]
    pair_parts = ((0, 1), (1, n_last - 1), (n_last, n_chip - n_last))

    def pair_sum(c, k):
        part = pl.ds(*pair_parts[k])
        return remote(psend.at[lax.rem(c, 2), part], precv.at[c, part], ps_s.at[c, k], ps_r.at[c, k], partner)

    def half_sum(way, c):
        rows = pl.ds(way * half, half)
        return remote(acc.at[c, hops, rows], rhalf.at[way, c], h_s.at[way, c], h_r.at[way, c], left if way else right)

    def full_sum(way, k, c):
        o = hops + k if way == 0 else hops - k
        return remote(acc.at[c, o], rfull.at[way, k - 1, c], f_s.at[way, k - 1, c], f_r.at[way, k - 1, c],
                      left if way else right)

    def down_chunk(c, last):
        load = c if last else c + n_col
        lo, hi = (bounds[2], n_chip) if last else (0, bounds[2])
        slot = lax.rem(load, WD_SLOTS)
        wd_copy(load).wait()
        for e in range(n_exp):
            rows = hid[e, pl.ds(lo * chip_cap, (hi - lo) * chip_cap), :]
            out = jnp.dot(rows, wd[slot, e], preferred_element_type=f32).astype(bf16)
            for p in range(lo, hi):
                ob[order[p], pl.ds(e * chip_cap, chip_cap), :] = out[(p - lo) * chip_cap:(p - lo + 1) * chip_cap]

        @pl.when(load + WD_SLOTS < 2 * n_col)
        def _():
            wd_copy(load + WD_SLOTS).start()

        @pl.when(c >= 2)
        def _():
            for k in (0, 1) if last else (2,):
                pair_sum(c - 2, k).wait_send()

        for q in range(n_last) if last else range(n_last, n_chip):
            o = far_first[q]
            got = jnp.dot(cmat[o], ob[o], preferred_element_type=f32)
            total = got[:LANES] + got[LANES:2 * LANES] + got[2 * LANES:]
            acc[c, o] = total[:tok]
            psend[lax.rem(c, 2), q] = total[tok:]
            if q == 0:
                pair_sum(c, 0).start()
        pair_sum(c, 1 if last else 2).start()

    def stage(k, c):
        if k == 0:
            pair_sum(c, 0).wait_recv()
            acc[c, hops] = acc[c, hops] + precv[c, 0]
            for way in range(2):
                half_sum(way, c).start()
            return
        if k < 3:
            pair_sum(c, k).wait_recv()
        if k == hops:
            total = acc[c, 0] + precv[c, far_first.index(0)]
            for way in range(2):
                full_sum(way, hops - 1, c).wait_recv()
                total = total + rfull[way, hops - 2, c]
            cols = pl.ds(pl.multiple_of(c * COLS, COLS), COLS)
            y_ref[:, cols] = total.astype(bf16)
            return
        for way in range(2):
            o = hops + k if way == 0 else hops - k
            acc[c, o] = acc[c, o] + precv[c, far_first.index(o)]
            if k == 1:
                half_sum(way, c).wait_recv()
                rows = pl.ds(way * half, half)
                acc[c, o, rows, :] = acc[c, o, rows, :] + rhalf[way, c]
            else:
                full_sum(way, k - 1, c).wait_recv()
                acc[c, o] = acc[c, o] + rfull[way, k - 2, c]
            full_sum(way, k, c).start()

    lag = n_col - 2

    def last_rows(i, carry):
        @pl.when(i < n_col)
        def _():
            down_chunk(i, True)

        @pl.when(i >= 1)
        def _():
            stage(0, i - 1)

        @pl.when(i >= lag)
        def _():
            stage(1, i - lag)
        return carry

    early = n_col + 1 - lag
    rest = n_col - early

    def first_rows(i, carry):
        down_chunk(i, False)

        @pl.when(i < rest)
        def _():
            stage(1, i + early)

        @pl.when(i >= rest)
        def _():
            stage(2, i - rest)
        return carry

    def finish(k, first):
        def one(c, carry):
            stage(k, c)
            return carry
        lax.fori_loop(first, n_col, one, 0)

    lax.fori_loop(0, n_col + 1, last_rows, 0)
    lax.fori_loop(0, n_col, first_rows, 0)
    finish(2, early)
    for k in range(3, hops + 1):
        finish(k, 0)

    for way in range(2):
        for j in range(n_step):
            ring_x(way, j).wait_send()
        for h in range(meta_hops[way]):
            ring_meta(way, h).wait_send()
    for o in range(n_chip):
        pair_meta(o).wait_send()
        for b in range(2):
            pair_x(o, b).wait_send()

    def drain(c, carry):
        for way in range(2):
            half_sum(way, c).wait_send()
            for k in range(1, hops):
                full_sum(way, k, c).wait_send()

        @pl.when(c >= n_col - 2)
        def _():
            for k in range(3):
                pair_sum(c, k).wait_send()
        return carry

    lax.fori_loop(0, n_col, drain, 0)


def solution(mesh):
    group = mesh.shape['expert']
    n_chip = group // 2
    hops = n_chip // 2

    def local_moe(x_loc, idx_loc, gate_loc, up_loc, down_loc):
        tok, d_model = x_loc.shape
        top_k = idx_loc.shape[1]
        n_exp, _, d_ff = up_loc.shape
        total_exp = n_exp * group
        cap = min(4, total_exp // top_k) * tok * top_k // total_exp
        n_col = d_model // COLS
        bf16, f32 = jnp.bfloat16, jnp.float32
        dma = pltpu.SemaphoreType.DMA
        any_spec = pl.BlockSpec(memory_space=pl.ANY)
        vmem_spec = pl.BlockSpec(memory_space=pltpu.VMEM)
        n_step = 2 * hops - 1
        return pl.pallas_call(
            functools.partial(moe_kernel, group, cap),
            out_shape=jax.ShapeDtypeStruct((tok, d_model), bf16),
            in_specs=[any_spec, vmem_spec, vmem_spec, any_spec, any_spec],
            out_specs=vmem_spec,
            scratch_shapes=[
                pltpu.VMEM((n_exp, d_model, d_ff), bf16),
                pltpu.VMEM((WD_SLOTS, n_exp, d_ff, COLS), bf16),
                pltpu.VMEM((n_chip, 2, tok, d_model), bf16),
                pltpu.VMEM((n_chip, 2, 16, LANES), f32),
                pltpu.VMEM((n_exp, n_chip * 2 * cap, d_model), bf16),
                pltpu.VMEM((n_exp, n_chip * 2 * cap, d_ff), bf16),
                pltpu.VMEM((n_chip, 3 * LANES, COLS), bf16),
                pltpu.VMEM((n_chip, COLS, COLS), bf16),
                pltpu.VMEM((n_col, n_chip, tok, COLS), f32),
                pltpu.VMEM((2, n_chip, tok, COLS), f32),
                pltpu.VMEM((n_col, n_chip, tok, COLS), f32),
                pltpu.VMEM((2, n_col, tok // 2, COLS), f32),
                pltpu.VMEM((2, hops - 1, n_col, tok, COLS), f32),
                dma, dma((n_exp,)), dma((WD_SLOTS,)),
                dma((2, n_step)), dma((2, n_step)), dma((2, hops)), dma((2, hops)),
                dma((n_chip, 2)), dma((n_chip, 2)), dma((n_chip,)), dma((n_chip,)),
                dma((n_col, 3)), dma((n_col, 3)), dma((2, n_col)), dma((2, n_col)),
                dma((2, hops - 1, n_col)), dma((2, hops - 1, n_col)),
            ],
            compiler_params=pltpu.CompilerParams(
                collective_id=0, has_side_effects=True, vmem_limit_bytes=67043328),
        )(x_loc, idx_loc.T, gate_loc.T, up_loc, down_loc)

    tok_spec = P(('data', 'expert'), None)
    w_spec = P('expert', None, None)
    return jax.shard_map(local_moe, mesh=mesh, in_specs=(tok_spec, tok_spec, tok_spec, w_spec, w_spec), out_specs=tok_spec, check_vma=False)
```

```python
import functools

import jax
import jax.numpy as jnp
from jax import lax
from jax.experimental import pallas as pl
from jax.experimental.pallas import tpu as pltpu
from jax.sharding import PartitionSpec as P

MESH = pl.DeviceIdType.MESH
COLS = 256
LANES = 128
WD_SLOTS = 5
PIECES = 4
ROW_CUTS = 4


def moe_kernel(group, cap, x_hbm, ids_ref, gate_ref, up_hbm, down_hbm, y_ref,
               wup, wd, xb, metab, xg, hid, cmat, ob, acc, psend, precv, rhalf, rfull,
               loc_sem, up_sem, wd_sem, ag_s, ag_r, mt_s, mt_r, pd_s, pd_r, pm_s, pm_r,
               ps_s, ps_r, h_s, h_r, f_s, f_r):
    n_chip = group // 2
    hops = n_chip // 2
    n_exp, d_model, d_ff = wup.shape
    tok = xb.shape[2]
    half = tok // 2
    chip_cap = 2 * cap
    slots = n_exp * chip_cap
    n_col = d_model // COLS
    f32, bf16 = jnp.float32, jnp.bfloat16

    me = lax.axis_index('expert')
    chip, core = me // 2, me % 2
    right = lax.rem(chip + 1, n_chip) * 2 + core
    left = lax.rem(chip + n_chip - 1, n_chip) * 2 + core
    partner = chip * 2 + 1 - core

    def remote(src, dst, send_sem, recv_sem, dev):
        return pltpu.make_async_remote_copy(src_ref=src, dst_ref=dst, send_sem=send_sem, recv_sem=recv_sem,
                                            device_id={'expert': dev}, device_id_type=MESH)

    x_copy = pltpu.make_async_copy(x_hbm, xb.at[0, 0], loc_sem)
    x_copy.start()
    top_k = ids_ref.shape[0]
    metab[0, 0] = jnp.full(metab.shape[2:], -1.0, f32)
    metab[0, 0, pl.ds(0, top_k), pl.ds(0, tok)] = ids_ref[...].astype(f32)
    metab[0, 0, pl.ds(8, top_k), pl.ds(0, tok)] = gate_ref[...]

    def up_copies(e):
        cut = d_model // ROW_CUTS
        return [pltpu.make_async_copy(up_hbm.at[e, pl.ds(r * cut, cut)], wup.at[e, pl.ds(r * cut, cut)], up_sem.at[e, r])
                for r in range(ROW_CUTS)]

    def wd_copies(load):
        slot = lax.rem(load, WD_SLOTS)
        cols = pl.ds(pl.multiple_of(lax.rem(load, n_col) * COLS, COLS), COLS)
        return [pltpu.make_async_copy(down_hbm.at[e, :, cols], wd.at[slot, e], wd_sem.at[slot, e]) for e in range(n_exp)]

    for e in range(n_exp):
        for copy in up_copies(e):
            copy.start()
    for c in range(WD_SLOTS):
        for copy in wd_copies(jnp.int32(c)):
            copy.start()

    barrier = pltpu.get_barrier_semaphore()
    for dev in (right, left, partner):
        pl.semaphore_signal(barrier, inc=1, device_id={'expert': dev}, device_id_type=MESH)
    pl.semaphore_wait(barrier, 3)
    x_copy.wait()

    steps = [[], []]
    for h in range(hops):
        for b in range(PIECES):
            for way in range(2):
                if h < hops - 1 or b // (PIECES // 2) == way:
                    steps[way].append((h, b))
    n_step = len(steps[0])
    piece = tok // PIECES

    def slot_of(way, h):
        return h if way == 0 else (n_chip - h) % n_chip

    def ring_x(way, j):
        h, b = steps[way][j]
        rows = pl.ds(b * piece, piece)
        return remote(xb.at[slot_of(way, h), 0, rows], xb.at[slot_of(way, h + 1), 0, rows],
                      ag_s.at[way, j], ag_r.at[way, j], left if way else right)

    def ring_meta(way, h):
        return remote(metab.at[slot_of(way, h), 0], metab.at[slot_of(way, h + 1), 0],
                      mt_s.at[way, h], mt_r.at[way, h], left if way else right)

    def pair_x(o, b):
        rows = pl.ds(b * piece, piece)
        return remote(xb.at[o, 0, rows], xb.at[o, 1, rows], pd_s.at[o, b], pd_r.at[o, b], partner)

    def pair_meta(o):
        return remote(metab.at[o, 0], metab.at[o, 1], pm_s.at[o], pm_r.at[o], partner)

    meta_hops = (hops, hops - 1)

    order = [0]
    for h in range(1, hops):
        order += [h, n_chip - h]
    order.append(hops)
    place = {o: p for p, o in enumerate(order)}
    bounds = [0, 3, 5, n_chip]
    held = [p if p < bounds[2] else p - bounds[2] for p in range(n_chip)]

    tri_r = lax.broadcasted_iota(jnp.int32, (LANES, LANES), 0)
    tri_c = lax.broadcasted_iota(jnp.int32, (LANES, LANES), 1)
    before = jnp.logical_and(tri_r < tri_c, (tri_r >= tok) == (tri_c >= tok))
    tri = jnp.where(before, 1.0, 0.0).astype(bf16)
    lane8 = lax.broadcasted_iota(jnp.int32, (8, LANES), 1)
    row8 = lax.broadcasted_iota(jnp.int32, (8, LANES), 0)
    slot_row = lax.broadcasted_iota(jnp.int32, (chip_cap, LANES), 0).astype(f32)

    def route(o):
        m0, m1 = metab[o, 0], metab[o, 1]
        low = lane8 < tok
        ids = jnp.where(low, m0[:8], pltpu.roll(m1[:8], tok, 1))
        gates = jnp.where(low, m0[8:], pltpu.roll(m1[8:], tok, 1))
        mask = jnp.zeros((8, LANES), f32)
        gate_rows = []
        for e in range(n_exp):
            hit = ids == (me * n_exp + e).astype(f32)
            row = jnp.sum(jnp.where(hit, 1.0, 0.0), axis=0, keepdims=True)
            mask = jnp.where(row8 == e, row, mask)
            gate_rows.append(jnp.sum(jnp.where(hit, gates, 0.0), axis=0, keepdims=True))
        pos = jnp.dot(mask.astype(bf16), tri, preferred_element_type=f32)
        pos = jnp.where(mask > 0.5, pos + jnp.where(low, 0.0, float(cap)), -1.0)
        pick = [jnp.where(slot_row == pos[e:e + 1, :], 1.0, 0.0) for e in range(n_exp)]
        pick_all = jnp.concatenate(pick, axis=0).astype(bf16)
        for n in range(d_model // COLS):
            cols = pl.ds(n * COLS, COLS)
            rows_x = jnp.concatenate([xb[o, 0, :, cols], xb[o, 1, :, cols]], axis=0)
            got = jnp.dot(pick_all, rows_x, preferred_element_type=f32).astype(bf16)
            for e in range(n_exp):
                xg[e, pl.ds(held[place[o]] * chip_cap, chip_cap), cols] = got[e * chip_cap:(e + 1) * chip_cap]
        weighted = [pick[e] * gate_rows[e] for e in range(n_exp)]
        weighted.append(jnp.zeros((COLS - slots, LANES), f32))
        rest = jnp.transpose(jnp.concatenate(weighted, axis=0))
        for part in range(3):
            piece = rest.astype(bf16)
            cmat[o, pl.ds(part * LANES, LANES), :] = piece
            rest = rest - piece.astype(f32)

    for way in range(2):
        ring_meta(way, 0).start()
    for j in range(PIECES):
        for way in range(2):
            ring_x(way, j).start()
    pair_meta(0).start()
    for b in range(PIECES):
        pair_x(0, b).start()

    def routed(o):
        pair_meta(o).wait_recv()
        for b in range(PIECES):
            pair_x(o, b).wait_recv()
        route(o)

    def gather_step(j):
        h = steps[0][j][0]
        if steps[0][j][1] == 0:
            for way in range(2):
                if h < meta_hops[way]:
                    ring_meta(way, h).wait_recv()
                    if h + 1 < meta_hops[way]:
                        ring_meta(way, h + 1).start()
                    pair_meta(slot_of(way, h + 1)).start()
        for way in range(2):
            ring_x(way, j).wait_recv()
            nxt = (steps[way][j][0] + 1, steps[way][j][1])
            if nxt in steps[way]:
                ring_x(way, steps[way].index(nxt)).start()
            pair_x(slot_of(way, h + 1), steps[way][j][1]).start()

    def up_rows(phase, e):
        if phase == 0:
            for copy in up_copies(e):
                copy.wait()
        lo, size = bounds[phase], (bounds[phase + 1] - bounds[phase]) * chip_cap
        src, dst = pl.ds(held[lo] * chip_cap, size), pl.ds(lo * chip_cap, size)
        for start in range(0, d_ff, COLS):
            cols = pl.ds(start, min(COLS, d_ff - start))
            raw = jnp.dot(xg[e, src, :], wup[e, :, cols], preferred_element_type=f32)
            hid[e, dst, cols] = jax.nn.gelu(raw, approximate=True).astype(bf16)

    far_first = order[::-1]
    work = [lambda: (routed(1), routed(n_chip - 1))]
    work += [functools.partial(up_rows, 0, e) for e in range(n_exp)]
    work += [lambda: (routed(2), routed(n_chip - 2))]
    work += [functools.partial(up_rows, 1, e) for e in range(n_exp)]
    routed(0)
    for j in range(n_step):
        gather_step(j)
        if j >= PIECES and work:
            work.pop(0)()
    for item in work:
        item()
    for p in range(bounds[2], n_chip):
        routed(order[p])
    for e in range(n_exp):
        up_rows(2, e)

    for o in range(n_chip):
        ob[o, pl.ds(slots, COLS - slots), :] = jnp.zeros((COLS - slots, COLS), bf16)

    n_last = n_chip - bounds[2]
    pair_parts = ((0, 1), (1, n_last - 1), (n_last, n_chip - n_last))

    def pair_sum(c, k):
        part = pl.ds(*pair_parts[k])
        return remote(psend.at[lax.rem(c, 2), part], precv.at[c, part], ps_s.at[c, k], ps_r.at[c, k], partner)

    def half_sum(way, c):
        rows = pl.ds(way * half, half)
        return remote(acc.at[c, hops, rows], rhalf.at[way, c], h_s.at[way, c], h_r.at[way, c], left if way else right)

    def full_sum(way, k, c):
        o = hops + k if way == 0 else hops - k
        return remote(acc.at[c, o], rfull.at[way, k - 1, c], f_s.at[way, k - 1, c], f_r.at[way, k - 1, c],
                      left if way else right)

    def down_chunk(c, last):
        load = c if last else c + n_col
        lo, hi = (bounds[2], n_chip) if last else (0, bounds[2])
        slot = lax.rem(load, WD_SLOTS)
        for copy in wd_copies(load):
            copy.wait()
        for e in range(n_exp):
            rows = hid[e, pl.ds(lo * chip_cap, (hi - lo) * chip_cap), :]
            out = jnp.dot(rows, wd[slot, e], preferred_element_type=f32).astype(bf16)
            for p in range(lo, hi):
                ob[order[p], pl.ds(e * chip_cap, chip_cap), :] = out[(p - lo) * chip_cap:(p - lo + 1) * chip_cap]

        @pl.when(load + WD_SLOTS < 2 * n_col)
        def _():
            for copy in wd_copies(load + WD_SLOTS):
                copy.start()

        @pl.when(c >= 2)
        def _():
            for k in (0, 1) if last else (2,):
                pair_sum(c - 2, k).wait_send()

        for q in range(n_last) if last else range(n_last, n_chip):
            o = far_first[q]
            got = jnp.dot(cmat[o], ob[o], preferred_element_type=f32)
            total = got[:LANES] + got[LANES:2 * LANES] + got[2 * LANES:]
            acc[c, o] = total[:tok]
            psend[lax.rem(c, 2), q] = total[tok:]
            if q == 0:
                pair_sum(c, 0).start()
        pair_sum(c, 1 if last else 2).start()

    def stage(k, c):
        if k == 0:
            pair_sum(c, 0).wait_recv()
            acc[c, hops] = acc[c, hops] + precv[c, 0]
            for way in range(2):
                half_sum(way, c).start()
            return
        if k < 3:
            pair_sum(c, k).wait_recv()
        if k == hops:
            total = acc[c, 0] + precv[c, far_first.index(0)]
            for way in range(2):
                full_sum(way, hops - 1, c).wait_recv()
                total = total + rfull[way, hops - 2, c]
            cols = pl.ds(pl.multiple_of(c * COLS, COLS), COLS)
            y_ref[:, cols] = total.astype(bf16)
            return
        for way in range(2):
            o = hops + k if way == 0 else hops - k
            acc[c, o] = acc[c, o] + precv[c, far_first.index(o)]
            if k == 1:
                half_sum(way, c).wait_recv()
                rows = pl.ds(way * half, half)
                acc[c, o, rows, :] = acc[c, o, rows, :] + rhalf[way, c]
            else:
                full_sum(way, k - 1, c).wait_recv()
                acc[c, o] = acc[c, o] + rfull[way, k - 2, c]
            full_sum(way, k, c).start()

    lag = n_col - 2

    def last_rows(i, carry):
        @pl.when(i < n_col)
        def _():
            down_chunk(i, True)

        @pl.when(i >= 1)
        def _():
            stage(0, i - 1)

        @pl.when(i >= lag)
        def _():
            stage(1, i - lag)
        return carry

    early = n_col + 1 - lag
    rest = n_col - early

    def first_rows(i, carry):
        down_chunk(i, False)

        @pl.when(i < rest)
        def _():
            stage(1, i + early)

        @pl.when(i >= rest)
        def _():
            stage(2, i - rest)
        return carry

    def finish(k, first):
        def one(c, carry):
            stage(k, c)
            return carry
        lax.fori_loop(first, n_col, one, 0)

    lax.fori_loop(0, n_col + 1, last_rows, 0)
    lax.fori_loop(0, n_col, first_rows, 0)
    finish(2, early)
    for k in range(3, hops + 1):
        finish(k, 0)

    for way in range(2):
        for j in range(n_step):
            ring_x(way, j).wait_send()
        for h in range(meta_hops[way]):
            ring_meta(way, h).wait_send()
    for o in range(n_chip):
        pair_meta(o).wait_send()
        for b in range(PIECES):
            pair_x(o, b).wait_send()

    def drain(c, carry):
        for way in range(2):
            half_sum(way, c).wait_send()
            for k in range(1, hops):
                full_sum(way, k, c).wait_send()

        @pl.when(c >= n_col - 2)
        def _():
            for k in range(3):
                pair_sum(c, k).wait_send()
        return carry

    lax.fori_loop(0, n_col, drain, 0)


def solution(mesh):
    group = mesh.shape['expert']
    n_chip = group // 2
    hops = n_chip // 2

    def local_moe(x_loc, idx_loc, gate_loc, up_loc, down_loc):
        tok, d_model = x_loc.shape
        top_k = idx_loc.shape[1]
        n_exp, _, d_ff = up_loc.shape
        total_exp = n_exp * group
        cap = min(4, total_exp // top_k) * tok * top_k // total_exp
        n_col = d_model // COLS
        bf16, f32 = jnp.bfloat16, jnp.float32
        dma = pltpu.SemaphoreType.DMA
        any_spec = pl.BlockSpec(memory_space=pl.ANY)
        vmem_spec = pl.BlockSpec(memory_space=pltpu.VMEM)
        n_step = PIECES * hops - PIECES // 2
        return pl.pallas_call(
            functools.partial(moe_kernel, group, cap),
            out_shape=jax.ShapeDtypeStruct((tok, d_model), bf16),
            in_specs=[any_spec, vmem_spec, vmem_spec, any_spec, any_spec],
            out_specs=vmem_spec,
            scratch_shapes=[
                pltpu.VMEM((n_exp, d_model, d_ff), bf16),
                pltpu.VMEM((WD_SLOTS, n_exp, d_ff, COLS), bf16),
                pltpu.VMEM((n_chip, 2, tok, d_model), bf16),
                pltpu.VMEM((n_chip, 2, 16, LANES), f32),
                pltpu.VMEM((n_exp, (n_chip - 3) * 2 * cap, d_model), bf16),
                pltpu.VMEM((n_exp, n_chip * 2 * cap, d_ff), bf16),
                pltpu.VMEM((n_chip, 3 * LANES, COLS), bf16),
                pltpu.VMEM((n_chip, COLS, COLS), bf16),
                pltpu.VMEM((n_col, n_chip, tok, COLS), f32),
                pltpu.VMEM((2, n_chip, tok, COLS), f32),
                pltpu.VMEM((n_col, n_chip, tok, COLS), f32),
                pltpu.VMEM((2, n_col, tok // 2, COLS), f32),
                pltpu.VMEM((2, hops - 1, n_col, tok, COLS), f32),
                dma, dma((n_exp, ROW_CUTS)), dma((WD_SLOTS, n_exp)),
                dma((2, n_step)), dma((2, n_step)), dma((2, hops)), dma((2, hops)),
                dma((n_chip, PIECES)), dma((n_chip, PIECES)), dma((n_chip,)), dma((n_chip,)),
                dma((n_col, 3)), dma((n_col, 3)), dma((2, n_col)), dma((2, n_col)),
                dma((2, hops - 1, n_col)), dma((2, hops - 1, n_col)),
            ],
            compiler_params=pltpu.CompilerParams(
                collective_id=0, has_side_effects=True, vmem_limit_bytes=67043328),
        )(x_loc, idx_loc.T, gate_loc.T, up_loc, down_loc)

    tok_spec = P(('data', 'expert'), None)
    w_spec = P('expert', None, None)
    return jax.shard_map(local_moe, mesh=mesh, in_specs=(tok_spec, tok_spec, tok_spec, w_spec, w_spec), out_specs=tok_spec, check_vma=False)
```

```python
import functools

import jax
import jax.numpy as jnp
from jax import lax
from jax.experimental import pallas as pl
from jax.experimental.pallas import tpu as pltpu
from jax.sharding import PartitionSpec as P

MESH = pl.DeviceIdType.MESH
COLS = 256
LANES = 128
WD_SLOTS = 5
PIECES = 4
ROW_CUTS = 1
DOWN_CUTS = 1


def moe_kernel(group, cap, x_hbm, ids_ref, gate_ref, up_hbm, down_hbm, y_ref,
               wup, wd, xb, metab, xg, hid, cmat, ob, acc, psend, precv, rhalf, rfull,
               loc_sem, up_sem, wd_sem, ag_s, ag_r, mt_s, mt_r, pd_s, pd_r, pm_s, pm_r,
               ps_s, ps_r, h_s, h_r, f_s, f_r):
    n_chip = group // 2
    hops = n_chip // 2
    n_exp, d_model, d_ff = wup.shape
    tok = xb.shape[2]
    half = tok // 2
    chip_cap = 2 * cap
    slots = n_exp * chip_cap
    n_col = d_model // COLS
    f32, bf16 = jnp.float32, jnp.bfloat16

    me = lax.axis_index('expert')
    chip, core = me // 2, me % 2
    right = lax.rem(chip + 1, n_chip) * 2 + core
    left = lax.rem(chip + n_chip - 1, n_chip) * 2 + core
    partner = chip * 2 + 1 - core

    def remote(src, dst, send_sem, recv_sem, dev):
        return pltpu.make_async_remote_copy(src_ref=src, dst_ref=dst, send_sem=send_sem, recv_sem=recv_sem,
                                            device_id={'expert': dev}, device_id_type=MESH)

    x_copy = pltpu.make_async_copy(x_hbm, xb.at[0, 0], loc_sem)
    x_copy.start()
    top_k = ids_ref.shape[0]
    metab[0, 0] = jnp.full(metab.shape[2:], -1.0, f32)
    metab[0, 0, pl.ds(0, top_k), pl.ds(0, tok)] = ids_ref[...].astype(f32)
    metab[0, 0, pl.ds(8, top_k), pl.ds(0, tok)] = gate_ref[...]

    def up_copies(e):
        cut = d_model // ROW_CUTS
        return [pltpu.make_async_copy(up_hbm.at[e, pl.ds(r * cut, cut)], wup.at[e, pl.ds(r * cut, cut)], up_sem.at[e, r])
                for r in range(ROW_CUTS)]

    def wd_copies(load):
        slot = lax.rem(load, WD_SLOTS)
        cols = pl.ds(pl.multiple_of(lax.rem(load, n_col) * COLS, COLS), COLS)
        cut = n_exp // DOWN_CUTS
        return [pltpu.make_async_copy(down_hbm.at[pl.ds(r * cut, cut), :, cols], wd.at[slot, pl.ds(r * cut, cut)], wd_sem.at[slot, r])
                for r in range(DOWN_CUTS)]

    for e in range(n_exp):
        for copy in up_copies(e):
            copy.start()

    barrier = pltpu.get_barrier_semaphore()
    for dev in (right, left, partner):
        pl.semaphore_signal(barrier, inc=1, device_id={'expert': dev}, device_id_type=MESH)
    pl.semaphore_wait(barrier, 3)
    x_copy.wait()

    steps = [[], []]
    for h in range(hops):
        for b in range(PIECES):
            for way in range(2):
                if h < hops - 1 or b // (PIECES // 2) == way:
                    steps[way].append((h, b))
    n_step = len(steps[0])
    piece = tok // PIECES

    def slot_of(way, h):
        return h if way == 0 else (n_chip - h) % n_chip

    def ring_x(way, j):
        h, b = steps[way][j]
        rows = pl.ds(b * piece, piece)
        return remote(xb.at[slot_of(way, h), 0, rows], xb.at[slot_of(way, h + 1), 0, rows],
                      ag_s.at[way, j], ag_r.at[way, j], left if way else right)

    def ring_meta(way, h):
        return remote(metab.at[slot_of(way, h), 0], metab.at[slot_of(way, h + 1), 0],
                      mt_s.at[way, h], mt_r.at[way, h], left if way else right)

    def pair_x(o, b):
        rows = pl.ds(b * piece, piece)
        return remote(xb.at[o, 0, rows], xb.at[o, 1, rows], pd_s.at[o, b], pd_r.at[o, b], partner)

    def pair_meta(o):
        return remote(metab.at[o, 0], metab.at[o, 1], pm_s.at[o], pm_r.at[o], partner)

    meta_hops = (hops, hops - 1)

    order = [0]
    for h in range(1, hops):
        order += [h, n_chip - h]
    order.append(hops)
    place = {o: p for p, o in enumerate(order)}
    bounds = [0, 3, 5, n_chip]
    held = [p if p < bounds[2] else p - bounds[2] for p in range(n_chip)]

    tri_r = lax.broadcasted_iota(jnp.int32, (LANES, LANES), 0)
    tri_c = lax.broadcasted_iota(jnp.int32, (LANES, LANES), 1)
    before = jnp.logical_and(tri_r < tri_c, (tri_r >= tok) == (tri_c >= tok))
    tri = jnp.where(before, 1.0, 0.0).astype(bf16)
    lane8 = lax.broadcasted_iota(jnp.int32, (8, LANES), 1)
    row8 = lax.broadcasted_iota(jnp.int32, (8, LANES), 0)
    slot_row = lax.broadcasted_iota(jnp.int32, (chip_cap, LANES), 0).astype(f32)

    def route(o):
        m0, m1 = metab[o, 0], metab[o, 1]
        low = lane8 < tok
        ids = jnp.where(low, m0[:8], pltpu.roll(m1[:8], tok, 1))
        gates = jnp.where(low, m0[8:], pltpu.roll(m1[8:], tok, 1))
        mask = jnp.zeros((8, LANES), f32)
        gate_rows = []
        for e in range(n_exp):
            hit = ids == (me * n_exp + e).astype(f32)
            row = jnp.sum(jnp.where(hit, 1.0, 0.0), axis=0, keepdims=True)
            mask = jnp.where(row8 == e, row, mask)
            gate_rows.append(jnp.sum(jnp.where(hit, gates, 0.0), axis=0, keepdims=True))
        pos = jnp.dot(mask.astype(bf16), tri, preferred_element_type=f32)
        pos = jnp.where(mask > 0.5, pos + jnp.where(low, 0.0, float(cap)), -1.0)
        pick = [jnp.where(slot_row == pos[e:e + 1, :], 1.0, 0.0) for e in range(n_exp)]
        pick_all = jnp.concatenate(pick, axis=0).astype(bf16)
        for n in range(d_model // COLS):
            cols = pl.ds(n * COLS, COLS)
            rows_x = jnp.concatenate([xb[o, 0, :, cols], xb[o, 1, :, cols]], axis=0)
            got = jnp.dot(pick_all, rows_x, preferred_element_type=f32).astype(bf16)
            for e in range(n_exp):
                xg[e, pl.ds(held[place[o]] * chip_cap, chip_cap), cols] = got[e * chip_cap:(e + 1) * chip_cap]
        weighted = [pick[e] * gate_rows[e] for e in range(n_exp)]
        weighted.append(jnp.zeros((COLS - slots, LANES), f32))
        rest = jnp.transpose(jnp.concatenate(weighted, axis=0))
        for part in range(3):
            piece = rest.astype(bf16)
            cmat[o, pl.ds(part * LANES, LANES), :] = piece
            rest = rest - piece.astype(f32)

    for way in range(2):
        ring_meta(way, 0).start()
    for j in range(PIECES):
        for way in range(2):
            ring_x(way, j).start()
    pair_meta(0).start()
    for b in range(PIECES):
        pair_x(0, b).start()

    def routed(o):
        pair_meta(o).wait_recv()
        for b in range(PIECES):
            pair_x(o, b).wait_recv()
        route(o)

    def gather_step(j):
        h = steps[0][j][0]
        if steps[0][j][1] == 0:
            for way in range(2):
                if h < meta_hops[way]:
                    ring_meta(way, h).wait_recv()
                    if h + 1 < meta_hops[way]:
                        ring_meta(way, h + 1).start()
                    pair_meta(slot_of(way, h + 1)).start()
        for way in range(2):
            ring_x(way, j).wait_recv()
            nxt = (steps[way][j][0] + 1, steps[way][j][1])
            if nxt in steps[way]:
                ring_x(way, steps[way].index(nxt)).start()
            pair_x(slot_of(way, h + 1), steps[way][j][1]).start()

    def start_down():
        for c in range(WD_SLOTS):
            for copy in wd_copies(jnp.int32(c)):
                copy.start()

    def up_rows(phase, e):
        if phase == 0:
            for copy in up_copies(e):
                copy.wait()
        lo, size = bounds[phase], (bounds[phase + 1] - bounds[phase]) * chip_cap
        src, dst = pl.ds(held[lo] * chip_cap, size), pl.ds(lo * chip_cap, size)
        for start in range(0, d_ff, COLS):
            cols = pl.ds(start, min(COLS, d_ff - start))
            raw = jnp.dot(xg[e, src, :], wup[e, :, cols], preferred_element_type=f32)
            hid[e, dst, cols] = jax.nn.gelu(raw, approximate=True).astype(bf16)

    far_first = order[::-1]
    first, second = [[functools.partial(up_rows, phase, e) for e in range(n_exp)] for phase in range(2)]

    def routed_both(h):
        routed(h)
        routed(n_chip - h)

    work = {4: [lambda: routed_both(1)], 5: first[:1], 6: first[1:3], 7: first[3:], 8: [start_down, lambda: routed_both(2), second[0]],
            9: second[1:2], 10: second[2:3], 11: second[3:], 12: [lambda: routed_both(3)]}
    routed(0)
    for j in range(n_step):
        gather_step(j)
        for item in work.get(j, ()):
            item()
    routed(hops)
    for e in range(n_exp):
        up_rows(2, e)

    for o in range(n_chip):
        ob[o, pl.ds(slots, COLS - slots), :] = jnp.zeros((COLS - slots, COLS), bf16)

    n_last = n_chip - bounds[2]
    pair_parts = ((0, 1), (1, n_last - 1), (n_last, n_chip - n_last))

    def pair_sum(c, k):
        part = pl.ds(*pair_parts[k])
        return remote(psend.at[lax.rem(c, 2), part], precv.at[c, part], ps_s.at[c, k], ps_r.at[c, k], partner)

    def half_sum(way, c):
        rows = pl.ds(way * half, half)
        return remote(acc.at[c, hops, rows], rhalf.at[way, c], h_s.at[way, c], h_r.at[way, c], left if way else right)

    def full_sum(way, k, c):
        o = hops + k if way == 0 else hops - k
        return remote(acc.at[c, o], rfull.at[way, k - 1, c], f_s.at[way, k - 1, c], f_r.at[way, k - 1, c],
                      left if way else right)

    def down_chunk(c, last):
        load = c if last else c + n_col
        lo, hi = (bounds[2], n_chip) if last else (0, bounds[2])
        slot = lax.rem(load, WD_SLOTS)
        for copy in wd_copies(load):
            copy.wait()
        for e in range(n_exp):
            rows = hid[e, pl.ds(lo * chip_cap, (hi - lo) * chip_cap), :]
            out = jnp.dot(rows, wd[slot, e], preferred_element_type=f32).astype(bf16)
            for p in range(lo, hi):
                ob[order[p], pl.ds(e * chip_cap, chip_cap), :] = out[(p - lo) * chip_cap:(p - lo + 1) * chip_cap]

        @pl.when(load + WD_SLOTS < 2 * n_col)
        def _():
            for copy in wd_copies(load + WD_SLOTS):
                copy.start()

        @pl.when(c >= 2)
        def _():
            for k in (0, 1) if last else (2,):
                pair_sum(c - 2, k).wait_send()

        for q in range(n_last) if last else range(n_last, n_chip):
            o = far_first[q]
            got = jnp.dot(cmat[o], ob[o], preferred_element_type=f32)
            total = got[:LANES] + got[LANES:2 * LANES] + got[2 * LANES:]
            acc[c, o] = total[:tok]
            psend[lax.rem(c, 2), q] = total[tok:]
            if q == 0:
                pair_sum(c, 0).start()
        pair_sum(c, 1 if last else 2).start()

    def stage(k, c):
        if k == 0:
            pair_sum(c, 0).wait_recv()
            acc[c, hops] = acc[c, hops] + precv[c, 0]
            for way in range(2):
                half_sum(way, c).start()
            return
        if k < 3:
            pair_sum(c, k).wait_recv()
        if k == hops:
            total = acc[c, 0] + precv[c, far_first.index(0)]
            for way in range(2):
                full_sum(way, hops - 1, c).wait_recv()
                total = total + rfull[way, hops - 2, c]
            cols = pl.ds(pl.multiple_of(c * COLS, COLS), COLS)
            y_ref[:, cols] = total.astype(bf16)
            return
        for way in range(2):
            o = hops + k if way == 0 else hops - k
            acc[c, o] = acc[c, o] + precv[c, far_first.index(o)]
            if k == 1:
                half_sum(way, c).wait_recv()
                rows = pl.ds(way * half, half)
                acc[c, o, rows, :] = acc[c, o, rows, :] + rhalf[way, c]
            else:
                full_sum(way, k - 1, c).wait_recv()
                acc[c, o] = acc[c, o] + rfull[way, k - 2, c]
            full_sum(way, k, c).start()

    lag = n_col - 2

    def last_rows(i, carry):
        @pl.when(i < n_col)
        def _():
            down_chunk(i, True)

        @pl.when(i >= 1)
        def _():
            stage(0, i - 1)

        @pl.when(i >= lag)
        def _():
            stage(1, i - lag)
        return carry

    early = n_col + 1 - lag
    rest = n_col - early

    def first_rows(i, carry):
        down_chunk(i, False)

        @pl.when(i < rest)
        def _():
            stage(1, i + early)

        @pl.when(i >= rest)
        def _():
            stage(2, i - rest)
        return carry

    def finish(k, first):
        def one(c, carry):
            stage(k, c)
            return carry
        lax.fori_loop(first, n_col, one, 0)

    lax.fori_loop(0, n_col + 1, last_rows, 0)
    lax.fori_loop(0, n_col, first_rows, 0)
    finish(2, early)
    for k in range(3, hops + 1):
        finish(k, 0)

    for way in range(2):
        for j in range(n_step):
            ring_x(way, j).wait_send()
        for h in range(meta_hops[way]):
            ring_meta(way, h).wait_send()
    for o in range(n_chip):
        pair_meta(o).wait_send()
        for b in range(PIECES):
            pair_x(o, b).wait_send()

    def drain(c, carry):
        for way in range(2):
            half_sum(way, c).wait_send()
            for k in range(1, hops):
                full_sum(way, k, c).wait_send()

        @pl.when(c >= n_col - 2)
        def _():
            for k in range(3):
                pair_sum(c, k).wait_send()
        return carry

    lax.fori_loop(0, n_col, drain, 0)


def solution(mesh):
    group = mesh.shape['expert']
    n_chip = group // 2
    hops = n_chip // 2

    def local_moe(x_loc, idx_loc, gate_loc, up_loc, down_loc):
        tok, d_model = x_loc.shape
        top_k = idx_loc.shape[1]
        n_exp, _, d_ff = up_loc.shape
        total_exp = n_exp * group
        cap = min(4, total_exp // top_k) * tok * top_k // total_exp
        n_col = d_model // COLS
        bf16, f32 = jnp.bfloat16, jnp.float32
        dma = pltpu.SemaphoreType.DMA
        any_spec = pl.BlockSpec(memory_space=pl.ANY)
        vmem_spec = pl.BlockSpec(memory_space=pltpu.VMEM)
        n_step = PIECES * hops - PIECES // 2
        return pl.pallas_call(
            functools.partial(moe_kernel, group, cap),
            out_shape=jax.ShapeDtypeStruct((tok, d_model), bf16),
            in_specs=[any_spec, vmem_spec, vmem_spec, any_spec, any_spec],
            out_specs=vmem_spec,
            scratch_shapes=[
                pltpu.VMEM((n_exp, d_model, d_ff), bf16),
                pltpu.VMEM((WD_SLOTS, n_exp, d_ff, COLS), bf16),
                pltpu.VMEM((n_chip, 2, tok, d_model), bf16),
                pltpu.VMEM((n_chip, 2, 16, LANES), f32),
                pltpu.VMEM((n_exp, (n_chip - 3) * 2 * cap, d_model), bf16),
                pltpu.VMEM((n_exp, n_chip * 2 * cap, d_ff), bf16),
                pltpu.VMEM((n_chip, 3 * LANES, COLS), bf16),
                pltpu.VMEM((n_chip, COLS, COLS), bf16),
                pltpu.VMEM((n_col, n_chip, tok, COLS), f32),
                pltpu.VMEM((2, n_chip, tok, COLS), f32),
                pltpu.VMEM((n_col, n_chip, tok, COLS), f32),
                pltpu.VMEM((2, n_col, tok // 2, COLS), f32),
                pltpu.VMEM((2, hops - 1, n_col, tok, COLS), f32),
                dma, dma((n_exp, ROW_CUTS)), dma((WD_SLOTS, DOWN_CUTS)),
                dma((2, n_step)), dma((2, n_step)), dma((2, hops)), dma((2, hops)),
                dma((n_chip, PIECES)), dma((n_chip, PIECES)), dma((n_chip,)), dma((n_chip,)),
                dma((n_col, 3)), dma((n_col, 3)), dma((2, n_col)), dma((2, n_col)),
                dma((2, hops - 1, n_col)), dma((2, hops - 1, n_col)),
            ],
            compiler_params=pltpu.CompilerParams(
                collective_id=0, has_side_effects=True, vmem_limit_bytes=67043328),
        )(x_loc, idx_loc.T, gate_loc.T, up_loc, down_loc)

    tok_spec = P(('data', 'expert'), None)
    w_spec = P('expert', None, None)
    return jax.shard_map(local_moe, mesh=mesh, in_specs=(tok_spec, tok_spec, tok_spec, w_spec, w_spec), out_specs=tok_spec, check_vma=False)
```

```python
import functools

import jax
import jax.numpy as jnp
from jax import lax
from jax.experimental import pallas as pl
from jax.experimental.pallas import tpu as pltpu
from jax.sharding import PartitionSpec as P

MESH = pl.DeviceIdType.MESH
COLS = 256
LANES = 128
WD_SLOTS = 5
PIECES = 4
UP_COLS = 768
ROW_CUTS = 1
DOWN_CUTS = 1


def moe_kernel(group, cap, x_hbm, ids_ref, gate_ref, up_hbm, down_hbm, y_ref,
               wup, wd, xb, metab, xg, hid, cmat, ob, acc, psend, precv, rhalf, rfull,
               loc_sem, up_sem, wd_sem, ag_s, ag_r, mt_s, mt_r, pd_s, pd_r, pm_s, pm_r,
               ps_s, ps_r, h_s, h_r, f_s, f_r):
    n_chip = group // 2
    hops = n_chip // 2
    n_exp, d_model, d_ff = wup.shape
    tok = xb.shape[2]
    half = tok // 2
    chip_cap = 2 * cap
    slots = n_exp * chip_cap
    n_col = d_model // COLS
    f32, bf16 = jnp.float32, jnp.bfloat16

    me = lax.axis_index('expert')
    chip, core = me // 2, me % 2
    right = lax.rem(chip + 1, n_chip) * 2 + core
    left = lax.rem(chip + n_chip - 1, n_chip) * 2 + core
    partner = chip * 2 + 1 - core

    def remote(src, dst, send_sem, recv_sem, dev):
        return pltpu.make_async_remote_copy(src_ref=src, dst_ref=dst, send_sem=send_sem, recv_sem=recv_sem,
                                            device_id={'expert': dev}, device_id_type=MESH)

    x_copy = pltpu.make_async_copy(x_hbm, xb.at[0, 0], loc_sem)
    x_copy.start()
    top_k = ids_ref.shape[0]
    metab[0, 0] = jnp.full(metab.shape[2:], -1.0, f32)
    metab[0, 0, pl.ds(0, top_k), pl.ds(0, tok)] = ids_ref[...].astype(f32)
    metab[0, 0, pl.ds(8, top_k), pl.ds(0, tok)] = gate_ref[...]

    def up_copies(e):
        cut = d_model // ROW_CUTS
        return [pltpu.make_async_copy(up_hbm.at[e, pl.ds(r * cut, cut)], wup.at[e, pl.ds(r * cut, cut)], up_sem.at[e, r])
                for r in range(ROW_CUTS)]

    def wd_copies(load):
        slot = lax.rem(load, WD_SLOTS)
        cols = pl.ds(pl.multiple_of(lax.rem(load, n_col) * COLS, COLS), COLS)
        cut = n_exp // DOWN_CUTS
        return [pltpu.make_async_copy(down_hbm.at[pl.ds(r * cut, cut), :, cols], wd.at[slot, pl.ds(r * cut, cut)], wd_sem.at[slot, r])
                for r in range(DOWN_CUTS)]

    for e in range(n_exp):
        for copy in up_copies(e):
            copy.start()

    barrier = pltpu.get_barrier_semaphore()
    for dev in (right, left, partner):
        pl.semaphore_signal(barrier, inc=1, device_id={'expert': dev}, device_id_type=MESH)
    pl.semaphore_wait(barrier, 3)
    x_copy.wait()

    steps = [[], []]
    for h in range(hops):
        for b in range(PIECES):
            for way in range(2):
                if h < hops - 1 or b // (PIECES // 2) == way:
                    steps[way].append((h, b))
    n_step = len(steps[0])
    piece = tok // PIECES

    def slot_of(way, h):
        return h if way == 0 else (n_chip - h) % n_chip

    def ring_x(way, j):
        h, b = steps[way][j]
        rows = pl.ds(b * piece, piece)
        return remote(xb.at[slot_of(way, h), 0, rows], xb.at[slot_of(way, h + 1), 0, rows],
                      ag_s.at[way, j], ag_r.at[way, j], left if way else right)

    def ring_meta(way, h):
        return remote(metab.at[slot_of(way, h), 0], metab.at[slot_of(way, h + 1), 0],
                      mt_s.at[way, h], mt_r.at[way, h], left if way else right)

    def pair_x(o, b):
        rows = pl.ds(b * piece, piece)
        return remote(xb.at[o, 0, rows], xb.at[o, 1, rows], pd_s.at[o, b], pd_r.at[o, b], partner)

    def pair_meta(o):
        return remote(metab.at[o, 0], metab.at[o, 1], pm_s.at[o], pm_r.at[o], partner)

    meta_hops = (hops, hops - 1)

    order = [0]
    for h in range(1, hops):
        order += [h, n_chip - h]
    order.append(hops)
    place = {o: p for p, o in enumerate(order)}
    bounds = [0, 3, 5, n_chip]
    held = [p if p < bounds[2] else p - bounds[2] for p in range(n_chip)]

    tri_r = lax.broadcasted_iota(jnp.int32, (LANES, LANES), 0)
    tri_c = lax.broadcasted_iota(jnp.int32, (LANES, LANES), 1)
    before = jnp.logical_and(tri_r < tri_c, (tri_r >= tok) == (tri_c >= tok))
    tri = jnp.where(before, 1.0, 0.0).astype(bf16)
    lane8 = lax.broadcasted_iota(jnp.int32, (8, LANES), 1)
    row8 = lax.broadcasted_iota(jnp.int32, (8, LANES), 0)
    slot_row = lax.broadcasted_iota(jnp.int32, (chip_cap, LANES), 0).astype(f32)

    def route(o):
        m0, m1 = metab[o, 0], metab[o, 1]
        low = lane8 < tok
        ids = jnp.where(low, m0[:8], pltpu.roll(m1[:8], tok, 1))
        gates = jnp.where(low, m0[8:], pltpu.roll(m1[8:], tok, 1))
        mask = jnp.zeros((8, LANES), f32)
        gate_rows = []
        for e in range(n_exp):
            hit = ids == (me * n_exp + e).astype(f32)
            row = jnp.sum(jnp.where(hit, 1.0, 0.0), axis=0, keepdims=True)
            mask = jnp.where(row8 == e, row, mask)
            gate_rows.append(jnp.sum(jnp.where(hit, gates, 0.0), axis=0, keepdims=True))
        pos = jnp.dot(mask.astype(bf16), tri, preferred_element_type=f32)
        pos = jnp.where(mask > 0.5, pos + jnp.where(low, 0.0, float(cap)), -1.0)
        pick = [jnp.where(slot_row == pos[e:e + 1, :], 1.0, 0.0) for e in range(n_exp)]
        pick_all = jnp.concatenate(pick, axis=0).astype(bf16)
        for n in range(d_model // COLS):
            cols = pl.ds(n * COLS, COLS)
            rows_x = jnp.concatenate([xb[o, 0, :, cols], xb[o, 1, :, cols]], axis=0)
            got = jnp.dot(pick_all, rows_x, preferred_element_type=f32).astype(bf16)
            for e in range(n_exp):
                xg[e, pl.ds(held[place[o]] * chip_cap, chip_cap), cols] = got[e * chip_cap:(e + 1) * chip_cap]
        weighted = [pick[e] * gate_rows[e] for e in range(n_exp)]
        weighted.append(jnp.zeros((COLS - slots, LANES), f32))
        rest = jnp.transpose(jnp.concatenate(weighted, axis=0))
        for part in range(3):
            piece = rest.astype(bf16)
            cmat[o, pl.ds(part * LANES, LANES), :] = piece
            rest = rest - piece.astype(f32)

    for way in range(2):
        ring_meta(way, 0).start()
    for j in range(PIECES):
        for way in range(2):
            ring_x(way, j).start()
    pair_meta(0).start()
    for b in range(PIECES):
        pair_x(0, b).start()

    def routed(o):
        pair_meta(o).wait_recv()
        for b in range(PIECES):
            pair_x(o, b).wait_recv()
        route(o)

    def gather_step(j):
        h = steps[0][j][0]
        if steps[0][j][1] == 0:
            for way in range(2):
                if h < meta_hops[way]:
                    ring_meta(way, h).wait_recv()
                    if h + 1 < meta_hops[way]:
                        ring_meta(way, h + 1).start()
                    pair_meta(slot_of(way, h + 1)).start()
        for way in range(2):
            ring_x(way, j).wait_recv()
            nxt = (steps[way][j][0] + 1, steps[way][j][1])
            if nxt in steps[way]:
                ring_x(way, steps[way].index(nxt)).start()
            pair_x(slot_of(way, h + 1), steps[way][j][1]).start()

    def start_down():
        for c in range(WD_SLOTS):
            for copy in wd_copies(jnp.int32(c)):
                copy.start()

    def up_rows(phase, e):
        if phase == 0:
            for copy in up_copies(e):
                copy.wait()
        lo, size = bounds[phase], (bounds[phase + 1] - bounds[phase]) * chip_cap
        src, dst = pl.ds(held[lo] * chip_cap, size), pl.ds(lo * chip_cap, size)
        for start in range(0, d_ff, UP_COLS):
            cols = pl.ds(start, min(UP_COLS, d_ff - start))
            raw = jnp.dot(xg[e, src, :], wup[e, :, cols], preferred_element_type=f32)
            hid[e, dst, cols] = jax.nn.gelu(raw, approximate=True).astype(bf16)

    far_first = order[::-1]
    first, second = [[functools.partial(up_rows, phase, e) for e in range(n_exp)] for phase in range(2)]

    def routed_both(h):
        routed(h)
        routed(n_chip - h)

    work = {4: [lambda: routed_both(1)], 5: first[:1], 6: first[1:3], 7: first[3:], 8: [start_down, lambda: routed_both(2), second[0]],
            9: second[1:2], 10: second[2:3], 11: second[3:], 12: [lambda: routed_both(3)]}
    routed(0)
    for j in range(n_step):
        gather_step(j)
        for item in work.get(j, ()):
            item()
    routed(hops)
    for e in range(n_exp):
        up_rows(2, e)

    for o in range(n_chip):
        ob[o, pl.ds(slots, COLS - slots), :] = jnp.zeros((COLS - slots, COLS), bf16)

    n_last = n_chip - bounds[2]
    pair_parts = ((0, 1), (1, n_last - 1), (n_last, n_chip - n_last))

    def pair_sum(c, k):
        part = pl.ds(*pair_parts[k])
        return remote(psend.at[lax.rem(c, 2), part], precv.at[c, part], ps_s.at[c, k], ps_r.at[c, k], partner)

    def half_sum(way, c):
        rows = pl.ds(way * half, half)
        return remote(acc.at[c, hops, rows], rhalf.at[way, c], h_s.at[way, c], h_r.at[way, c], left if way else right)

    def full_sum(way, k, c):
        o = hops + k if way == 0 else hops - k
        return remote(acc.at[c, o], rfull.at[way, k - 1, c], f_s.at[way, k - 1, c], f_r.at[way, k - 1, c],
                      left if way else right)

    def down_chunk(c, last):
        load = c if last else c + n_col
        lo, hi = (bounds[2], n_chip) if last else (0, bounds[2])
        slot = lax.rem(load, WD_SLOTS)
        for copy in wd_copies(load):
            copy.wait()
        for e in range(n_exp):
            rows = hid[e, pl.ds(lo * chip_cap, (hi - lo) * chip_cap), :]
            out = jnp.dot(rows, wd[slot, e], preferred_element_type=f32).astype(bf16)
            for p in range(lo, hi):
                ob[order[p], pl.ds(e * chip_cap, chip_cap), :] = out[(p - lo) * chip_cap:(p - lo + 1) * chip_cap]

        @pl.when(load + WD_SLOTS < 2 * n_col)
        def _():
            for copy in wd_copies(load + WD_SLOTS):
                copy.start()

        @pl.when(c >= 2)
        def _():
            for k in (0, 1) if last else (2,):
                pair_sum(c - 2, k).wait_send()

        for q in range(n_last) if last else range(n_last, n_chip):
            o = far_first[q]
            got = jnp.dot(cmat[o], ob[o], preferred_element_type=f32)
            total = got[:LANES] + got[LANES:2 * LANES] + got[2 * LANES:]
            acc[c, o] = total[:tok]
            psend[lax.rem(c, 2), q] = total[tok:]
            if q == 0:
                pair_sum(c, 0).start()
        pair_sum(c, 1 if last else 2).start()

    def stage(k, c):
        if k == 0:
            pair_sum(c, 0).wait_recv()
            acc[c, hops] = acc[c, hops] + precv[c, 0]
            for way in range(2):
                half_sum(way, c).start()
            return
        if k < 3:
            pair_sum(c, k).wait_recv()
        if k == hops:
            total = acc[c, 0] + precv[c, far_first.index(0)]
            for way in range(2):
                full_sum(way, hops - 1, c).wait_recv()
                total = total + rfull[way, hops - 2, c]
            cols = pl.ds(pl.multiple_of(c * COLS, COLS), COLS)
            y_ref[:, cols] = total.astype(bf16)
            return
        for way in range(2):
            o = hops + k if way == 0 else hops - k
            acc[c, o] = acc[c, o] + precv[c, far_first.index(o)]
            if k == 1:
                half_sum(way, c).wait_recv()
                rows = pl.ds(way * half, half)
                acc[c, o, rows, :] = acc[c, o, rows, :] + rhalf[way, c]
            else:
                full_sum(way, k - 1, c).wait_recv()
                acc[c, o] = acc[c, o] + rfull[way, k - 2, c]
            full_sum(way, k, c).start()

    lag = n_col - 2

    def last_rows(i, carry):
        @pl.when(i < n_col)
        def _():
            down_chunk(i, True)

        @pl.when(i >= 1)
        def _():
            stage(0, i - 1)

        @pl.when(i >= lag)
        def _():
            stage(1, i - lag)
        return carry

    early = n_col + 1 - lag
    rest = n_col - early

    def first_rows(i, carry):
        down_chunk(i, False)

        @pl.when(i < rest)
        def _():
            stage(1, i + early)

        @pl.when(i >= rest)
        def _():
            stage(2, i - rest)
        return carry

    def finish(k, first):
        def one(c, carry):
            stage(k, c)
            return carry
        lax.fori_loop(first, n_col, one, 0)

    lax.fori_loop(0, n_col + 1, last_rows, 0)
    lax.fori_loop(0, n_col, first_rows, 0)
    finish(2, early)
    for k in range(3, hops + 1):
        finish(k, 0)

    for way in range(2):
        for j in range(n_step):
            ring_x(way, j).wait_send()
        for h in range(meta_hops[way]):
            ring_meta(way, h).wait_send()
    for o in range(n_chip):
        pair_meta(o).wait_send()
        for b in range(PIECES):
            pair_x(o, b).wait_send()

    def drain(c, carry):
        for way in range(2):
            half_sum(way, c).wait_send()
            for k in range(1, hops):
                full_sum(way, k, c).wait_send()

        @pl.when(c >= n_col - 2)
        def _():
            for k in range(3):
                pair_sum(c, k).wait_send()
        return carry

    lax.fori_loop(0, n_col, drain, 0)


def solution(mesh):
    group = mesh.shape['expert']
    n_chip = group // 2
    hops = n_chip // 2

    def local_moe(x_loc, idx_loc, gate_loc, up_loc, down_loc):
        tok, d_model = x_loc.shape
        top_k = idx_loc.shape[1]
        n_exp, _, d_ff = up_loc.shape
        total_exp = n_exp * group
        cap = min(4, total_exp // top_k) * tok * top_k // total_exp
        n_col = d_model // COLS
        bf16, f32 = jnp.bfloat16, jnp.float32
        dma = pltpu.SemaphoreType.DMA
        any_spec = pl.BlockSpec(memory_space=pl.ANY)
        vmem_spec = pl.BlockSpec(memory_space=pltpu.VMEM)
        n_step = PIECES * hops - PIECES // 2
        return pl.pallas_call(
            functools.partial(moe_kernel, group, cap),
            out_shape=jax.ShapeDtypeStruct((tok, d_model), bf16),
            in_specs=[any_spec, vmem_spec, vmem_spec, any_spec, any_spec],
            out_specs=vmem_spec,
            scratch_shapes=[
                pltpu.VMEM((n_exp, d_model, d_ff), bf16),
                pltpu.VMEM((WD_SLOTS, n_exp, d_ff, COLS), bf16),
                pltpu.VMEM((n_chip, 2, tok, d_model), bf16),
                pltpu.VMEM((n_chip, 2, 16, LANES), f32),
                pltpu.VMEM((n_exp, (n_chip - 3) * 2 * cap, d_model), bf16),
                pltpu.VMEM((n_exp, n_chip * 2 * cap, d_ff), bf16),
                pltpu.VMEM((n_chip, 3 * LANES, COLS), bf16),
                pltpu.VMEM((n_chip, COLS, COLS), bf16),
                pltpu.VMEM((n_col, n_chip, tok, COLS), f32),
                pltpu.VMEM((2, n_chip, tok, COLS), f32),
                pltpu.VMEM((n_col, n_chip, tok, COLS), f32),
                pltpu.VMEM((2, n_col, tok // 2, COLS), f32),
                pltpu.VMEM((2, hops - 1, n_col, tok, COLS), f32),
                dma, dma((n_exp, ROW_CUTS)), dma((WD_SLOTS, DOWN_CUTS)),
                dma((2, n_step)), dma((2, n_step)), dma((2, hops)), dma((2, hops)),
                dma((n_chip, PIECES)), dma((n_chip, PIECES)), dma((n_chip,)), dma((n_chip,)),
                dma((n_col, 3)), dma((n_col, 3)), dma((2, n_col)), dma((2, n_col)),
                dma((2, hops - 1, n_col)), dma((2, hops - 1, n_col)),
            ],
            compiler_params=pltpu.CompilerParams(
                collective_id=0, has_side_effects=True, vmem_limit_bytes=67043328),
        )(x_loc, idx_loc.T, gate_loc.T, up_loc, down_loc)

    tok_spec = P(('data', 'expert'), None)
    w_spec = P('expert', None, None)
    return jax.shard_map(local_moe, mesh=mesh, in_specs=(tok_spec, tok_spec, tok_spec, w_spec, w_spec), out_specs=tok_spec, check_vma=False)
```
